32 devices in a mesh: epoch: 4 (over y, x), blend: 8 (over z, core).
Axes of the slice: x: 2, y: 2, z: 4, core: 2. Of those that a mesh axis runs over, the one named last changes fastest.
Arguments:
- visit_flux: bfloat16 [16, 32, 6, 16384], P('epoch', None, None, 'blend'), may hold values from -6 to 6
- visit_precision: bfloat16 [16, 32, 6, 16384], P('epoch', None, None, 'blend'), may hold values from 0.25 to 4
- visit_live: int32 [16, 32], P('epoch'), may hold values 0 or 1
- footprint: int32 [32, 8, 16384], P('blend', None, 'epoch'), may hold values 0 or 1
- source_count: int32 [32], P('blend'), may hold values from 1 to 8
- spectra_init: float32 [32, 8, 6], P('blend'), may hold values from 0.2 to 1.2
- morphology_init: float32 [32, 8, 16384], P('blend', None, 'epoch'), may hold values from 0 to 0.25
Outputs:
- coadd_flux: float32 [32, 6, 16384], P('blend', None, 'epoch')
- spectra: float32 [32, 8, 6], P('blend')
- morphology: float32 [32, 8, 16384], P('blend', None, 'epoch')
The draws below stay inside these ranges and needn't reach their ends.
All inputs are finite; a program needn't handle non-finite values. No bound on the sum of `visit_live` or of `footprint` on one device may be relied on, other than what follows from the above.
Results may differ from the reference program's by a relative error of at most 0.0003.
Values sent between devices are 32-bit elements; how exact they have to be, the bound alone decides.
No kernel may reach another device: no remote copies, remote signals or barrier semaphores. Data moves between devices by JAX's collectives and lax.ppermute only.
A program may use at most 64 MiB of HBM per device.

```python
import math
import jax
import jax.numpy as jnp
from jax import lax

PIX = 16384
BANDS = 6
SRC = 8
ITERS = 2
EPOCHS = 16
BLENDS = 32


def with_ends(array, key, smallest, largest):
    dims = array.shape
    place = [jax.random.randint(jax.random.fold_in(key, axis), (), 0, dims[axis]) for axis in range(len(dims))]
    array = array.at[tuple(place)].set(smallest)
    longest = dims.index(max(dims))
    place[longest] = (place[longest] + 1) % dims[longest]
    return array.at[tuple(place)].set(largest)


def shard_levels(rng, shape, pieces, low, top_value):
    def one(position, blocks):
        draws = jax.random.uniform(jax.random.fold_in(jax.random.fold_in(rng, 6), position), (blocks,), jnp.float32, low / len(pieces), top_value / len(pieces))
        return jnp.repeat(jnp.exp(draws), shape[position] // blocks).reshape((-1,) + (1,) * (len(shape) - position - 1))

    gain = one(*pieces[0])
    for cut in pieces[1:]:
        gain = gain * one(*cut)
    return gain


def normal_values(own_key, extent, spread, bound, pieces=(), held_as=jnp.bfloat16):
    loudness = shard_levels(own_key, extent, pieces, -0.22, 0.18) if pieces else 1.0
    result = jax.random.normal(own_key, extent, jnp.float32) * spread * loudness
    return jnp.minimum(jnp.maximum(result, -bound), bound).astype(held_as)


def setup_inputs(seed: int = 0) -> dict:
    key_of = jax.random.split(jax.random.key(seed), 8)
    return {
        "visit_flux": normal_values(key_of[0], (EPOCHS, BLENDS, BANDS, PIX), 1.0, 6.0, ((0, 4), (3, 8))),
        "visit_precision": jnp.clip(jnp.exp(math.log(4.0) - 2.7725887 * jax.random.uniform(key_of[1], (EPOCHS, BLENDS, BANDS, PIX), jnp.float32) ** shard_levels(key_of[1], (EPOCHS, BLENDS, BANDS, PIX), ((0, 4), (3, 8)), -0.2, 0.2)), 0.25, 4.0).astype(jnp.bfloat16),
        "visit_live": with_ends((jax.random.randint(key_of[2], (EPOCHS, BLENDS), 0, 4) < 3).astype(jnp.int32), jax.random.fold_in(key_of[2], 1), 0, 1),
        "footprint": with_ends((jax.random.randint(key_of[3], (BLENDS, SRC, PIX), 0, 2) < 1).astype(jnp.int32), jax.random.fold_in(key_of[3], 1), 0, 1),
        "source_count": with_ends(jax.random.randint(key_of[4], (BLENDS,), 1, SRC + 1), jax.random.fold_in(key_of[4], 1), 1, SRC).astype(jnp.int32),
        "spectra_init": jnp.clip(0.2 + 1 * jax.random.uniform(key_of[5], (BLENDS, SRC, BANDS), jnp.float32) ** shard_levels(key_of[5], (BLENDS, SRC, BANDS), ((0, 8),), -0.2, 0.2), 0.2, 1.2),
        "morphology_init": jnp.clip(0.25 * jax.random.uniform(key_of[6], (BLENDS, SRC, PIX), jnp.float32) ** shard_levels(key_of[6], (BLENDS, SRC, PIX), ((0, 8), (2, 4)), -0.2, 0.2), 0.0, 0.25),
    }


def reference(visit_flux, visit_precision, visit_live, footprint, source_count, spectra_init, morphology_init):
    def accumulate(totals, visit):
        flux_one, precision_one, live_one = visit
        weights = precision_one.astype(jnp.float32) * live_one.astype(jnp.float32)[:, None, None]
        return (totals[0] + weights * flux_one.astype(jnp.float32), totals[1] + weights), None

    zeros = jnp.zeros(visit_flux.shape[1:], jnp.float32)
    (numerator, weight_sum), _ = lax.scan(accumulate, (zeros, zeros), (visit_flux, visit_precision, visit_live))
    coadd_flux = numerator / (1.0 + weight_sum)
    coverage = weight_sum / (1.0 + weight_sum)
    source_live = (jnp.arange(SRC, dtype=jnp.int32)[None, :] < source_count[:, None]).astype(jnp.float32)
    footprint_mask = footprint.astype(jnp.float32) * source_live[:, :, None]
    live_count = source_count.astype(jnp.float32)
    morphology = morphology_init * footprint_mask
    spectra = spectra_init
    highest = lax.Precision.HIGHEST
    for iteration in range(ITERS):
        blend_model = jnp.einsum("bkc,bkp->bcp", spectra, morphology, precision=highest)
        residual = coverage * (coadd_flux - blend_model)
        morph_grad = jnp.einsum("bkc,bcp->bkp", spectra, residual, precision=highest)
        morph_step = 1.0 / (1.0 + live_count[:, None] * jnp.sum(spectra * spectra, axis=2))
        morphology = jnp.maximum(0.0, morphology + morph_grad * morph_step[:, :, None]) * footprint_mask
        blend_model = jnp.einsum("bkc,bkp->bcp", spectra, morphology, precision=highest)
        residual = coverage * (coadd_flux - blend_model)
        spectra_grad = jnp.einsum("bkp,bcp->bkc", morphology, residual, precision=highest)
        morph_norm = jnp.sum(morphology * morphology, axis=2)
        spectra = jnp.maximum(0.0, spectra + spectra_grad / (1.0 + live_count[:, None] * morph_norm)[:, :, None])
    return coadd_flux, spectra, morphology
```

```python
import functools

import jax
import jax.numpy as jnp
from jax import lax
from jax.experimental import pallas as pl
from jax.experimental.pallas import tpu as pltpu
from jax.sharding import PartitionSpec as P

ITERS = 2
LANES = 128


def on_device_general(
    visit_flux, visit_precision, visit_live, footprint, source_count, spectra_init, morphology_init
):
    weights = visit_precision.astype(jnp.float32) * visit_live.astype(jnp.float32)[:, :, None, None]
    numerator = jnp.sum(weights * visit_flux.astype(jnp.float32), axis=0)
    weight_sum = jnp.sum(weights, axis=0)
    pix_part = morphology_init.shape[2]
    owned = morphology_init.shape[0]
    numerator, weight_sum = (
        lax.psum_scatter(numerator, "epoch", scatter_dimension=2, tiled=True),
        lax.psum_scatter(weight_sum, "epoch", scatter_dimension=2, tiled=True),
    )
    every_blend, band_count, piece = numerator.shape
    numerator = numerator.reshape(every_blend, band_count, 1, piece)
    weight_sum = weight_sum.reshape(every_blend, band_count, 1, piece)
    numerator, weight_sum = (
        lax.all_to_all(numerator, "blend", split_axis=0, concat_axis=2, tiled=True),
        lax.all_to_all(weight_sum, "blend", split_axis=0, concat_axis=2, tiled=True),
    )
    blocks = numerator.shape[2]
    numerator = numerator.reshape(owned, band_count, blocks, 1, piece)
    weight_sum = weight_sum.reshape(owned, band_count, blocks, 1, piece)
    numerator, weight_sum = (
        lax.all_to_all(numerator, "epoch", split_axis=2, concat_axis=3, tiled=True),
        lax.all_to_all(weight_sum, "epoch", split_axis=2, concat_axis=3, tiled=True),
    )
    numerator = numerator.reshape(owned, band_count, pix_part)
    weight_sum = weight_sum.reshape(owned, band_count, pix_part)
    coadd_flux = numerator / (1.0 + weight_sum)
    coverage = weight_sum / (1.0 + weight_sum)
    slots = footprint.shape[1]
    source_live = (jnp.arange(slots, dtype=jnp.int32)[None, :] < source_count[:, None]).astype(
        jnp.float32
    )
    footprint_mask = footprint.astype(jnp.float32) * source_live[:, :, None]
    live_count = source_count.astype(jnp.float32)
    morphology = morphology_init * footprint_mask
    spectra = spectra_init
    highest = lax.Precision.HIGHEST
    for iteration in range(ITERS):
        blend_model = jnp.einsum("bkc,bkp->bcp", spectra, morphology, precision=highest)
        residual = coverage * (coadd_flux - blend_model)
        morph_grad = jnp.einsum("bkc,bcp->bkp", spectra, residual, precision=highest)
        morph_step = 1.0 / (1.0 + live_count[:, None] * jnp.sum(spectra * spectra, axis=2))
        morphology = (
            jnp.maximum(0.0, morphology + morph_grad * morph_step[:, :, None]) * footprint_mask
        )
        blend_model = jnp.einsum("bkc,bkp->bcp", spectra, morphology, precision=highest)
        residual = coverage * (coadd_flux - blend_model)
        spectra_grad = jnp.einsum("bkp,bcp->bkc", morphology, residual, precision=highest)
        morph_norm = jnp.sum(morphology * morphology, axis=2)
        spectra_grad, morph_norm = lax.psum((spectra_grad, morph_norm), "epoch")
        spectra = jnp.maximum(
            0.0, spectra + spectra_grad / (1.0 + live_count[:, None] * morph_norm)[:, :, None]
        )
    return (coadd_flux, spectra, morphology)


def any_spec():
    return pl.BlockSpec(memory_space=pltpu.VMEM)


def cost(flops, nbytes):
    return pl.CostEstimate(flops=int(flops), bytes_accessed=int(nbytes), transcendentals=0)


def visit_sums(ids, flux, prec, live, ks, dims):
    epochs, bands, _, pix = flux.shape
    group, n_e = dims
    rows = pix // LANES
    block_rows = 2 * bands * rows
    half = n_e // 2
    order = {0: ((1, 3), (0, 2)), 1: ((2, 3), (0, 1))}

    def kernel(ids_ref, flux_ref, prec_ref, live_ref, s0, k0, s1, k1, scr):
        chip, e, c = ids_ref[pl.program_id(0)], ids_ref[len(ks)], ids_ref[len(ks) + 1]
        sub = lax.broadcasted_iota(jnp.int32, (group, live_ref.shape[1]), 0)
        lane = lax.broadcasted_iota(jnp.int32, (group, live_ref.shape[1]), 1)
        pick = lane == sub + chip * group
        lives = []
        for ep in range(epochs):
            row = live_ref[ep : ep + 1, :].astype(jnp.float32)
            col = jnp.sum(jnp.where(pick, jnp.broadcast_to(row, pick.shape), 0.0), axis=1, keepdims=True)
            lives.append(jnp.broadcast_to(col, (group, LANES)))
        for band in range(bands):
            for j in range(rows):
                at = pl.ds(j * LANES, LANES)
                num = wsum = None
                for ep in range(epochs):
                    w = prec_ref[ep, band, :, at].astype(jnp.float32) * lives[ep]
                    n = w * flux_ref[ep, band, :, at].astype(jnp.float32)
                    num = n if num is None else num + n
                    wsum = w if wsum is None else wsum + w
                scr[pl.ds(band * rows + j, group, stride=block_rows), :] = num
                scr[pl.ds((bands + band) * rows + j, group, stride=block_rows), :] = wsum
        for d, refs in ((0, (s0, k0)), (1, (s1, k1))):
            for ref, slots in zip(refs, order[d]):
                for i, p in enumerate(slots):
                    r = jnp.bitwise_xor(c, d) * n_e + jnp.bitwise_xor(e, p)
                    start = pl.multiple_of(r * block_rows, 8)
                    ref[0, i] = scr[pl.ds(start, block_rows), :].reshape(2 * bands, rows, LANES)

    out = jax.ShapeDtypeStruct((len(ks), half, 2 * bands, rows, LANES), jnp.float32)
    out_spec = pl.BlockSpec((1, half, 2 * bands, rows, LANES), lambda i, s: (i, 0, 0, 0, 0))
    in_spec = pl.BlockSpec((epochs, bands, group, pix), lambda i, s: (0, 0, s[i], 0))
    n_in = len(ks) * epochs * bands * group * pix
    return pl.pallas_call(
        kernel,
        grid_spec=pltpu.PrefetchScalarGridSpec(
            num_scalar_prefetch=1,
            grid=(len(ks),),
            in_specs=[in_spec, in_spec, any_spec()],
            out_specs=[out_spec] * 4,
            scratch_shapes=[pltpu.VMEM((group * block_rows, LANES), jnp.float32)],
        ),
        out_shape=[out] * 4,
        cost_estimate=cost(n_in * 6, n_in * 4 + n_in * 2),
        name="visit_sums",
    )(ids, flux, prec, live)


def coadd_kernel(ids, pieces, bands, n_e):
    n_b = len(pieces)
    rows = pieces[0].shape[1]
    total = n_b * rows
    per_e = total // n_e

    def kernel(ids_ref, *refs):
        ins, cov, outs, scr = refs[:n_b], refs[n_b], refs[n_b + 1 : n_b + 1 + n_e], refs[-1]
        e, b = ids_ref[0], ids_ref[1]
        for m in range(n_b):
            start = pl.multiple_of(jnp.bitwise_xor(b, m) * rows, 8)
            for band in range(bands):
                num, wsum = ins[m][band], ins[m][bands + band]
                inv = 1.0 / (1.0 + wsum)
                cov[band, pl.ds(start, rows), :] = wsum * inv
                scr[band, pl.ds(start, rows), :] = num * inv
        for p in range(n_e):
            start = pl.multiple_of(jnp.bitwise_xor(e, p) * per_e, 8)
            for band in range(bands):
                outs[p][band] = scr[band, pl.ds(start, per_e), :]

    return pl.pallas_call(
        kernel,
        in_specs=[pl.BlockSpec(memory_space=pltpu.SMEM)] + [any_spec()] * n_b,
        out_specs=[any_spec()] * (1 + n_e),
        out_shape=[jax.ShapeDtypeStruct((bands, total, LANES), jnp.float32)]
        + [jax.ShapeDtypeStruct((bands, per_e, LANES), jnp.float32)] * n_e,
        scratch_shapes=[pltpu.VMEM((bands, total, LANES), jnp.float32)],
        cost_estimate=cost(bands * total * LANES * 8, bands * total * LANES * 16),
        name="coadd",
    )(ids, *pieces)


def deblend_kernel(ids, cov, coadds, morphs, masks, spectra):
    n_e = len(coadds)
    bands, total, _ = cov.shape
    slots, lanes = morphs[0].shape
    per_e = lanes // LANES
    groups = total // 8

    def kernel(ids_ref, cov_ref, *refs):
        co_in, mo_in, ma_in = refs[:n_e], refs[n_e : 2 * n_e], refs[2 * n_e : 3 * n_e]
        spec_ref = refs[3 * n_e]
        outs = refs[3 * n_e + 1 : 4 * n_e + 1]
        spec_out = refs[4 * n_e + 1]
        co, mo, ma, res, acc, spec, step = refs[4 * n_e + 2 :]
        e, count = ids_ref[0], ids_ref[2]
        n_live = count.astype(jnp.float32)
        k_iota = lax.broadcasted_iota(jnp.int32, (slots, LANES), 0)
        live = (k_iota < count).astype(jnp.float32)
        for p in range(n_e):
            start = jnp.bitwise_xor(e, p) * per_e
            for band in range(bands):
                co[band, pl.ds(pl.multiple_of(start, 8), per_e), :] = co_in[p][band]
            for j in range(per_e):
                at = pl.ds(j * LANES, LANES)
                mask = ma_in[p][:, at].astype(jnp.float32) * live
                ma[pl.ds(start + j, slots, stride=total), :] = mask
                mo[pl.ds(start + j, slots, stride=total), :] = mo_in[p][:, at] * mask
        spec[...] = spec_ref[...]

        def bcast(ref, row):
            return jnp.broadcast_to(ref[pl.ds(row, 1), :], (8, LANES))

        for it in range(ITERS):
            square = None
            for band in range(bands):
                s = spec[pl.ds(band * slots, slots), :]
                square = s * s if square is None else square + s * s
            step[...] = 1.0 / (1.0 + n_live * square)

            def group(g, carry):
                at = pl.multiple_of(g * 8, 8)
                m = [mo[pl.ds(pl.multiple_of(k * total + at, 8), 8), :] for k in range(slots)]
                cv = [cov_ref[c, pl.ds(at, 8), :] for c in range(bands)]
                cd = [co[c, pl.ds(at, 8), :] for c in range(bands)]
                r = []
                for c in range(bands):
                    model = None
                    for k in range(slots):
                        t = bcast(spec, c * slots + k) * m[k]
                        model = t if model is None else model + t
                    r.append(cv[c] * (cd[c] - model))
                for k in range(slots):
                    grad = None
                    for c in range(bands):
                        t = bcast(spec, c * slots + k) * r[c]
                        grad = t if grad is None else grad + t
                    mk = ma[pl.ds(pl.multiple_of(k * total + at, 8), 8), :]
                    m[k] = jnp.maximum(0.0, m[k] + grad * bcast(step, k)) * mk
                    mo[pl.ds(pl.multiple_of(k * total + at, 8), 8), :] = m[k]
                for c in range(bands):
                    model = None
                    for k in range(slots):
                        t = bcast(spec, c * slots + k) * m[k]
                        model = t if model is None else model + t
                    res[c, pl.ds(at, 8), :] = cv[c] * (cd[c] - model)
                return carry

            lax.fori_loop(0, groups, group, 0)
            for k in range(slots):
                sums = [None] * (bands + 1)
                for g in range(groups):
                    m = mo[pl.ds(k * total + g * 8, 8), :]
                    for c in range(bands):
                        t = m * res[c, pl.ds(g * 8, 8), :]
                        sums[c] = t if sums[c] is None else sums[c] + t
                    t = m * m
                    sums[bands] = t if sums[bands] is None else sums[bands] + t
                for c in range(bands + 1):
                    acc[pl.ds((c * slots + k) * 8, 8), :] = sums[c]

            def reduced(c):
                v = None
                for s in range(8):
                    t = acc[pl.ds(c * slots * 8 + s, slots, stride=8), :]
                    v = t if v is None else v + t
                return jnp.broadcast_to(jnp.sum(v, axis=1, keepdims=True), (slots, LANES))

            den = 1.0 + n_live * reduced(bands)
            for c in range(bands):
                s = spec[pl.ds(c * slots, slots), :]
                spec[pl.ds(c * slots, slots), :] = jnp.maximum(0.0, s + reduced(c) / den)

        lane = lax.broadcasted_iota(jnp.int32, (slots, LANES), 1)
        tile = jnp.zeros((slots, LANES), jnp.float32)
        for c in range(bands):
            tile = jnp.where(lane == c, spec[pl.ds(c * slots, slots), :], tile)
        spec_out[...] = tile
        for p in range(n_e):
            start = jnp.bitwise_xor(e, p) * per_e
            for j in range(per_e):
                at = pl.ds(j * LANES, LANES)
                outs[p][0:slots, at] = mo[pl.ds(start + j, slots, stride=total), :]

    f32 = jnp.float32
    return pl.pallas_call(
        kernel,
        in_specs=[pl.BlockSpec(memory_space=pltpu.SMEM)] + [any_spec()] * (3 * n_e + 2),
        out_specs=[any_spec()] * (n_e + 1),
        out_shape=[jax.ShapeDtypeStruct((slots, lanes), f32)] * n_e
        + [jax.ShapeDtypeStruct((slots, LANES), f32)],
        scratch_shapes=[
            pltpu.VMEM((bands, total, LANES), f32),
            pltpu.VMEM((slots * total, LANES), f32),
            pltpu.VMEM((slots * total, LANES), f32),
            pltpu.VMEM((bands, total, LANES), f32),
            pltpu.VMEM(((bands + 1) * slots * 8, LANES), f32),
            pltpu.VMEM((bands * slots, LANES), f32),
            pltpu.VMEM((slots, LANES), f32),
        ],
        cost_estimate=cost(total * LANES * slots * bands * 8 * ITERS, total * LANES * 4 * 30),
        name="deblend",
    )(ids, cov, *coadds, *morphs, *masks, spectra)


def place_coadd(ids, pieces):
    n_e = len(pieces)
    bands, rows, _ = pieces[0].shape

    def kernel(ids_ref, *refs):
        ins, out, scr = refs[:n_e], refs[n_e], refs[n_e + 1]
        e = ids_ref[0]
        for p in range(n_e):
            scr[jnp.bitwise_xor(e, p)] = ins[p][...].reshape(bands * rows, LANES)
        for band in range(bands):
            for j in range(rows):
                for q in range(n_e):
                    out[band, q : q + 1, pl.ds(j * LANES, LANES)] = scr[q, pl.ds(band * rows + j, 1), :]

    return pl.pallas_call(
        kernel,
        in_specs=[pl.BlockSpec(memory_space=pltpu.SMEM)] + [any_spec()] * n_e,
        out_specs=any_spec(),
        out_shape=jax.ShapeDtypeStruct((bands, n_e, rows * LANES), jnp.float32),
        scratch_shapes=[pltpu.VMEM((n_e, bands * rows, LANES), jnp.float32)],
        cost_estimate=cost(bands * n_e * rows * LANES, bands * n_e * rows * LANES * 8),
        name="place_coadd",
    )(ids, *pieces)


def place_morph(ids, pieces, tiles, bands):
    n_e = len(pieces)
    slots, lanes = pieces[0].shape

    def kernel(ids_ref, *refs):
        ins, sp, out, spec = refs[:n_e], refs[n_e : 2 * n_e], refs[2 * n_e], refs[2 * n_e + 1]
        e = ids_ref[0]
        for p in range(n_e):
            q = jnp.bitwise_xor(e, p)
            out[q] = ins[p][...]
            spec[q] = sp[p][...]

    return pl.pallas_call(
        kernel,
        in_specs=[pl.BlockSpec(memory_space=pltpu.SMEM)] + [any_spec()] * (2 * n_e),
        out_specs=[any_spec()] * 2,
        out_shape=[
            jax.ShapeDtypeStruct((n_e, slots, lanes), jnp.float32),
            jax.ShapeDtypeStruct((n_e, slots, LANES), jnp.float32),
        ],
        cost_estimate=cost(n_e * slots * lanes, n_e * slots * lanes * 8),
        name="place_morph",
    )(ids, *pieces, *tiles)


def xor_permute(x, axis, size, mask):
    return lax.ppermute(x, axis, [(i, i ^ mask) for i in range(size)])


def on_device_blend(
    n_e, n_b, visit_flux, visit_precision, visit_live, footprint, source_count, spectra_init, morphology_init
):
    f32 = jnp.float32
    owned, slots, _ = morphology_init.shape
    bands = visit_flux.shape[2]
    cores = 2
    group = cores * owned
    e, b = lax.axis_index("epoch"), lax.axis_index("blend")
    chip, core = b // cores, b % cores
    flux = jnp.transpose(visit_flux, (0, 2, 1, 3))
    prec = jnp.transpose(visit_precision, (0, 2, 1, 3))

    def pick(x, p):
        return lax.dynamic_index_in_dim(x, e ^ p, 0, keepdims=False)

    def swap(xs):
        return [xs[0]] + [xor_permute(xs[p], "epoch", n_e, p) for p in range(1, n_e)]

    morphs = swap([pick(morphology_init, p) for p in range(n_e)])
    masks = swap([pick(footprint, p) for p in range(n_e)])
    count = pick(source_count, 0)
    spectra = jnp.transpose(pick(spectra_init, 0)).reshape(bands * slots, 1)
    spectra = jnp.broadcast_to(spectra, (bands * slots, LANES))
    ids = jnp.stack([e, b, count]).astype(jnp.int32)

    chips = n_b // cores
    chunks = [[k] for k in range(chips - 1, 1, -1)] + [[1, 0] if chips > 1 else [0]]
    pieces = [None] * n_b
    for ks in chunks:
        where = jnp.stack([chip ^ k for k in ks] + [e, core]).astype(jnp.int32)
        s0, k0, s1, k1 = visit_sums(where, flux, prec, visit_live, ks, (group, n_e))
        for d, (send, keep, first, second) in enumerate(((s0, k0, 1, 2), (s1, k1, 2, 1))):
            got = xor_permute(send, "epoch", n_e, first)
            onward = xor_permute(keep[:, 1] + got[:, 1], "epoch", n_e, second)
            full = keep[:, 0] + got[:, 0] + onward
            for i, k in enumerate(ks):
                m = k * cores + d
                pieces[m] = xor_permute(full[i], "blend", n_b, m) if m else full[i]
    cov, *coadds = coadd_kernel(ids, pieces, bands, n_e)
    *blocks, tile = deblend_kernel(ids, cov, coadds, morphs, masks, spectra)
    out_coadd = place_coadd(ids, swap(coadds))
    blocks = swap(blocks)
    tiles = swap([tile] * n_e)
    out_morph, out_spec = place_morph(ids, blocks, tiles, bands)
    return (jnp.transpose(out_coadd, (1, 0, 2)), out_spec[:, :, :bands], out_morph)


def solution(mesh):
    n_e, n_b = mesh.shape["epoch"], mesh.shape["blend"]
    in_specs = (
        P("epoch", None, None, "blend"),
        P("epoch", None, None, "blend"),
        P("epoch", None),
        P("blend", None, "epoch"),
        P("blend"),
        P("blend", None, None),
        P("blend", None, "epoch"),
    )
    out_specs = (P("blend", None, "epoch"), P("blend", None, None), P("blend", None, "epoch"))

    def on_device(*args):
        owned, slots, pix_part = args[6].shape
        pix = args[0].shape[3]
        by_blend = (
            n_e == 4
            and owned == n_e
            and slots == 8
            and n_b % 2 == 0
            and n_b & (n_b - 1) == 0
            and pix % (8 * LANES) == 0
            and pix_part % pix == 0
            and pix_part % (8 * LANES) == 0
        )
        if by_blend:
            return on_device_blend(n_e, n_b, *args)
        return on_device_general(*args)

    return jax.shard_map(
        on_device, mesh=mesh, in_specs=in_specs, out_specs=out_specs, check_vma=False
    )
```

```python
import jax
import jax.numpy as jnp
from jax import lax
from jax.experimental import pallas as pl
from jax.experimental.pallas import tpu as pltpu
from jax.sharding import PartitionSpec as P


ITERS = 2
LANES = 128


def on_device_general(
    visit_flux, visit_precision, visit_live, footprint, source_count, spectra_init, morphology_init
):
    weights = visit_precision.astype(jnp.float32) * visit_live.astype(jnp.float32)[:, :, None, None]
    numerator = jnp.sum(weights * visit_flux.astype(jnp.float32), axis=0)
    weight_sum = jnp.sum(weights, axis=0)
    pix_part = morphology_init.shape[2]
    owned = morphology_init.shape[0]
    numerator, weight_sum = (
        lax.psum_scatter(numerator, "epoch", scatter_dimension=2, tiled=True),
        lax.psum_scatter(weight_sum, "epoch", scatter_dimension=2, tiled=True),
    )
    every_blend, band_count, piece = numerator.shape
    numerator = numerator.reshape(every_blend, band_count, 1, piece)
    weight_sum = weight_sum.reshape(every_blend, band_count, 1, piece)
    numerator, weight_sum = (
        lax.all_to_all(numerator, "blend", split_axis=0, concat_axis=2, tiled=True),
        lax.all_to_all(weight_sum, "blend", split_axis=0, concat_axis=2, tiled=True),
    )
    blocks = numerator.shape[2]
    numerator = numerator.reshape(owned, band_count, blocks, 1, piece)
    weight_sum = weight_sum.reshape(owned, band_count, blocks, 1, piece)
    numerator, weight_sum = (
        lax.all_to_all(numerator, "epoch", split_axis=2, concat_axis=3, tiled=True),
        lax.all_to_all(weight_sum, "epoch", split_axis=2, concat_axis=3, tiled=True),
    )
    numerator = numerator.reshape(owned, band_count, pix_part)
    weight_sum = weight_sum.reshape(owned, band_count, pix_part)
    coadd_flux = numerator / (1.0 + weight_sum)
    coverage = weight_sum / (1.0 + weight_sum)
    slots = footprint.shape[1]
    source_live = (jnp.arange(slots, dtype=jnp.int32)[None, :] < source_count[:, None]).astype(
        jnp.float32
    )
    footprint_mask = footprint.astype(jnp.float32) * source_live[:, :, None]
    live_count = source_count.astype(jnp.float32)
    morphology = morphology_init * footprint_mask
    spectra = spectra_init
    highest = lax.Precision.HIGHEST
    for _ in range(ITERS):
        blend_model = jnp.einsum("bkc,bkp->bcp", spectra, morphology, precision=highest)
        residual = coverage * (coadd_flux - blend_model)
        morph_grad = jnp.einsum("bkc,bcp->bkp", spectra, residual, precision=highest)
        morph_step = 1.0 / (1.0 + live_count[:, None] * jnp.sum(spectra * spectra, axis=2))
        morphology = (
            jnp.maximum(0.0, morphology + morph_grad * morph_step[:, :, None]) * footprint_mask
        )
        blend_model = jnp.einsum("bkc,bkp->bcp", spectra, morphology, precision=highest)
        residual = coverage * (coadd_flux - blend_model)
        spectra_grad = jnp.einsum("bkp,bcp->bkc", morphology, residual, precision=highest)
        morph_norm = jnp.sum(morphology * morphology, axis=2)
        spectra_grad, morph_norm = lax.psum((spectra_grad, morph_norm), "epoch")
        spectra = jnp.maximum(
            0.0, spectra + spectra_grad / (1.0 + live_count[:, None] * morph_norm)[:, :, None]
        )
    return (coadd_flux, spectra, morphology)


VMEM_LIMIT = 8 * 1024 * 1024


def hbm(x):
    return pltpu.with_memory_space_constraint(x, pltpu.HBM)


def whole():
    return pl.BlockSpec(memory_space=pltpu.VMEM)


def in_place():
    return pl.BlockSpec(memory_space=pltpu.HBM)


def cost(flops, nbytes):
    return pl.CostEstimate(flops=int(flops), bytes_accessed=int(nbytes), transcendentals=0)


def params(limit=VMEM_LIMIT):
    return pltpu.CompilerParams(vmem_limit_bytes=limit)


def visit_sums(flux, prec, live, ks, owned, n_e, cores):
    epochs, bands, blends, pix = flux.shape
    group = cores * owned
    rows = pix // LANES
    block_rows = 2 * bands * rows
    half = n_e // 2
    n_k = len(ks)
    order = {0: ((1, 3), (0, 2)), 1: ((2, 3), (0, 1))}

    def kernel(live_ref, flux_ref, prec_ref, s0, k0, s1, k1, scr, fbuf, pbuf, sems):
        e, b = lax.axis_index("epoch"), lax.axis_index("blend")
        chip, c = b // cores, b % cores

        def copies(i, band):
            at = pl.ds(pl.multiple_of((chip ^ ks[i]) * group, 8), group)
            return [
                pltpu.make_async_copy(ref.at[:, band, at, :], buf.at[i, band], sems.at[i, band, n])
                for n, (ref, buf) in enumerate(((flux_ref, fbuf), (prec_ref, pbuf)))
            ]

        for i in range(n_k):
            for band in range(bands):
                for copy in copies(i, band):
                    copy.start()
        sub = lax.broadcasted_iota(jnp.int32, (group, blends), 0)
        lane = lax.broadcasted_iota(jnp.int32, (group, blends), 1)
        for i in range(n_k):
            pick = lane == sub + (chip ^ ks[i]) * group
            lives = []
            for ep in range(epochs):
                row = live_ref[ep : ep + 1, :].astype(jnp.float32)
                col = jnp.where(pick, jnp.broadcast_to(row, pick.shape), 0.0)
                lives.append(jnp.broadcast_to(jnp.sum(col, axis=1, keepdims=True), (group, LANES)))
            for band in range(bands):
                for copy in copies(i, band):
                    copy.wait()
                for j in range(rows):
                    at = pl.ds(j * LANES, LANES)
                    num = wsum = None
                    for ep in range(epochs):
                        w = pbuf[i, band, ep, :, at].astype(jnp.float32) * lives[ep]
                        n = w * fbuf[i, band, ep, :, at].astype(jnp.float32)
                        num = n if num is None else num + n
                        wsum = w if wsum is None else wsum + w
                    scr[pl.ds(band * rows + j, group, stride=block_rows), :] = num
                    scr[pl.ds((bands + band) * rows + j, group, stride=block_rows), :] = wsum
            for d, refs in ((0, (s0, k0)), (1, (s1, k1))):
                for ref, slots in zip(refs, order[d]):
                    for slot, p in enumerate(slots):
                        r = jnp.bitwise_xor(c, d) * n_e + jnp.bitwise_xor(e, p)
                        start = pl.multiple_of(r * block_rows, 8)
                        ref[slot, i] = scr[pl.ds(start, block_rows), :].reshape(2 * bands, rows, LANES)

    out = pltpu.VMEM((half, n_k, 2 * bands, rows, LANES), jnp.float32)
    n_in = n_k * epochs * bands * group * pix
    return pl.pallas_call(
        kernel,
        in_specs=[whole(), in_place(), in_place()],
        out_specs=[whole()] * 4,
        out_shape=[out] * 4,
        scratch_shapes=[
            pltpu.VMEM((group * block_rows, LANES), jnp.float32),
            pltpu.VMEM((n_k, bands, epochs, group, pix), flux.dtype),
            pltpu.VMEM((n_k, bands, epochs, group, pix), prec.dtype),
            pltpu.SemaphoreType.DMA((n_k, bands, 2)),
        ],
        compiler_params=params(),
        cost_estimate=cost(n_in * 6, n_in * 4 + n_in * 2),
        name="visit_sums",
    )(live, flux, prec)


def pack_kernel(morph, footprint, n_e):
    _, slots, lanes = morph.shape

    def kernel(morph_ref, foot_ref, *refs):
        outs, buf, sems = refs[:n_e], refs[n_e], refs[n_e + 1]
        e = lax.axis_index("epoch")
        copies = []
        for p in range(n_e):
            q = jnp.bitwise_xor(e, p)
            copies.append(
                (
                    pltpu.make_async_copy(morph_ref.at[q], outs[p].at[0], sems.at[p, 0]),
                    pltpu.make_async_copy(foot_ref.at[q], buf.at[p], sems.at[p, 1]),
                )
            )
        for pair in copies:
            for copy in pair:
                copy.start()
        for p, pair in enumerate(copies):
            for copy in pair:
                copy.wait()
            outs[p][1] = buf[p].astype(jnp.float32)

    n = n_e * slots * lanes
    return pl.pallas_call(
        kernel,
        in_specs=[in_place()] * 2,
        out_specs=[whole()] * n_e,
        out_shape=[pltpu.VMEM((2, slots, lanes), jnp.float32)] * n_e,
        scratch_shapes=[
            pltpu.VMEM((n_e, slots, lanes), footprint.dtype),
            pltpu.SemaphoreType.DMA((n_e, 2)),
        ],
        compiler_params=params(),
        cost_estimate=cost(n * 2, n * 16),
        name="pack",
    )(morph, footprint)


def coadd_kernel(pieces, bands, n_e):
    n_b = len(pieces)
    rows = pieces[0].shape[1]
    total = n_b * rows
    per_e = total // n_e

    def kernel(*refs):
        ins, cov, outs, scr = refs[:n_b], refs[n_b], refs[n_b + 1 : n_b + 1 + n_e], refs[-1]
        e, b = lax.axis_index("epoch"), lax.axis_index("blend")
        for m in range(n_b):
            start = pl.multiple_of(jnp.bitwise_xor(b, m) * rows, 8)
            for band in range(bands):
                num, wsum = ins[m][band], ins[m][bands + band]
                inv = 1.0 / (1.0 + wsum)
                cov[band, pl.ds(start, rows), :] = wsum * inv
                scr[band, pl.ds(start, rows), :] = num * inv
        for p in range(n_e):
            start = pl.multiple_of(jnp.bitwise_xor(e, p) * per_e, 8)
            for band in range(bands):
                outs[p][band] = scr[band, pl.ds(start, per_e), :]

    return pl.pallas_call(
        kernel,
        in_specs=[whole()] * n_b,
        out_specs=[whole()] * (1 + n_e),
        out_shape=[jax.ShapeDtypeStruct((bands, total, LANES), jnp.float32)]
        + [jax.ShapeDtypeStruct((bands, per_e, LANES), jnp.float32)] * n_e,
        scratch_shapes=[pltpu.VMEM((bands, total, LANES), jnp.float32)],
        compiler_params=params(),
        cost_estimate=cost(bands * total * LANES * 8, bands * total * LANES * 16),
        name="coadd",
    )(*pieces)


def deblend_kernel(counts, cov, coadds, packed, spectra):
    n_e = len(coadds)
    bands, total, _ = cov.shape
    _, slots, lanes = packed[0].shape
    per_e = lanes // LANES
    groups = total // 8

    def kernel(count_ref, cov_ref, *refs):
        co_in, pk_in = refs[:n_e], refs[n_e : 2 * n_e]
        spec_ref = refs[2 * n_e]
        outs = refs[2 * n_e + 1 : 3 * n_e + 1]
        co, mo, ma, res, acc, spec, step = refs[3 * n_e + 1 :]
        e = lax.axis_index("epoch")
        count = count_ref[e]
        n_live = count.astype(jnp.float32)
        k_iota = lax.broadcasted_iota(jnp.int32, (slots, LANES), 0)
        live = (k_iota < count).astype(jnp.float32)
        for p in range(n_e):
            start = jnp.bitwise_xor(e, p) * per_e
            for band in range(bands):
                co[band, pl.ds(pl.multiple_of(start, 8), per_e), :] = co_in[p][band]
            for j in range(per_e):
                at = pl.ds(j * LANES, LANES)
                mask = pk_in[p][1, :, at] * live
                ma[pl.ds(start + j, slots, stride=total), :] = mask
                mo[pl.ds(start + j, slots, stride=total), :] = pk_in[p][0, :, at] * mask
        spec[...] = spec_ref[...]

        def bcast(ref, row):
            return jnp.broadcast_to(ref[pl.ds(row, 1), :], (8, LANES))

        for _ in range(ITERS):
            square = None
            for band in range(bands):
                s = spec[pl.ds(band * slots, slots), :]
                square = s * s if square is None else square + s * s
            step[...] = 1.0 / (1.0 + n_live * square)

            def group(g, carry):
                at = pl.multiple_of(g * 8, 8)
                m = [mo[pl.ds(pl.multiple_of(k * total + at, 8), 8), :] for k in range(slots)]
                cv = [cov_ref[c, pl.ds(at, 8), :] for c in range(bands)]
                cd = [co[c, pl.ds(at, 8), :] for c in range(bands)]
                r = []
                for c in range(bands):
                    model = None
                    for k in range(slots):
                        t = bcast(spec, c * slots + k) * m[k]
                        model = t if model is None else model + t
                    r.append(cv[c] * (cd[c] - model))
                for k in range(slots):
                    grad = None
                    for c in range(bands):
                        t = bcast(spec, c * slots + k) * r[c]
                        grad = t if grad is None else grad + t
                    mk = ma[pl.ds(pl.multiple_of(k * total + at, 8), 8), :]
                    m[k] = jnp.maximum(0.0, m[k] + grad * bcast(step, k)) * mk
                    mo[pl.ds(pl.multiple_of(k * total + at, 8), 8), :] = m[k]
                for c in range(bands):
                    model = None
                    for k in range(slots):
                        t = bcast(spec, c * slots + k) * m[k]
                        model = t if model is None else model + t
                    res[c, pl.ds(at, 8), :] = cv[c] * (cd[c] - model)
                return carry

            lax.fori_loop(0, groups, group, 0)
            for k in range(slots):
                sums = [None] * (bands + 1)
                for g in range(groups):
                    m = mo[pl.ds(k * total + g * 8, 8), :]
                    for c in range(bands):
                        t = m * res[c, pl.ds(g * 8, 8), :]
                        sums[c] = t if sums[c] is None else sums[c] + t
                    t = m * m
                    sums[bands] = t if sums[bands] is None else sums[bands] + t
                for c in range(bands + 1):
                    acc[pl.ds((c * slots + k) * 8, 8), :] = sums[c]

            def reduced(c):
                v = None
                for s in range(8):
                    t = acc[pl.ds(c * slots * 8 + s, slots, stride=8), :]
                    v = t if v is None else v + t
                return jnp.broadcast_to(jnp.sum(v, axis=1, keepdims=True), (slots, LANES))

            den = 1.0 + n_live * reduced(bands)
            for c in range(bands):
                s = spec[pl.ds(c * slots, slots), :]
                spec[pl.ds(c * slots, slots), :] = jnp.maximum(0.0, s + reduced(c) / den)

        lane = lax.broadcasted_iota(jnp.int32, (slots, LANES), 1)
        tile = jnp.zeros((slots, LANES), jnp.float32)
        for c in range(bands):
            on_diag = jnp.where(lane == k_iota, spec[pl.ds(c * slots, slots), :], 0.0)
            row = jnp.broadcast_to(jnp.sum(on_diag, axis=0, keepdims=True), (slots, LANES))
            tile = jnp.where(k_iota == c, row, tile)
        for p in range(n_e):
            start = jnp.bitwise_xor(e, p) * per_e
            for j in range(per_e):
                outs[p][:, pl.ds(j * LANES, LANES)] = mo[pl.ds(start + j, slots, stride=total), :]
            outs[p][:, pl.ds(lanes, LANES)] = tile

    f32 = jnp.float32
    return pl.pallas_call(
        kernel,
        in_specs=[pl.BlockSpec(memory_space=pltpu.SMEM)] + [whole()] * (2 * n_e + 2),
        out_specs=[whole()] * n_e,
        out_shape=[jax.ShapeDtypeStruct((slots, lanes + LANES), f32)] * n_e,
        scratch_shapes=[
            pltpu.VMEM((bands, total, LANES), f32),
            pltpu.VMEM((slots * total, LANES), f32),
            pltpu.VMEM((slots * total, LANES), f32),
            pltpu.VMEM((bands, total, LANES), f32),
            pltpu.VMEM(((bands + 1) * slots * 8, LANES), f32),
            pltpu.VMEM((bands * slots, LANES), f32),
            pltpu.VMEM((slots, LANES), f32),
        ],
        compiler_params=params(),
        cost_estimate=cost(total * LANES * slots * bands * 8 * ITERS, total * LANES * 4 * 30),
        name="deblend",
    )(counts, cov, *coadds, *packed, spectra)


def place_coadd(pieces):
    n_e = len(pieces)
    bands, rows, _ = pieces[0].shape

    def kernel(*refs):
        ins, out, scr = refs[:n_e], refs[n_e], refs[n_e + 1]
        e = lax.axis_index("epoch")
        for p in range(n_e):
            scr[jnp.bitwise_xor(e, p)] = ins[p][...].reshape(bands * rows, LANES)
        for band in range(bands):
            for j in range(rows):
                for q in range(n_e):
                    out[band, q : q + 1, pl.ds(j * LANES, LANES)] = scr[q, pl.ds(band * rows + j, 1), :]

    return pl.pallas_call(
        kernel,
        in_specs=[whole()] * n_e,
        out_specs=whole(),
        out_shape=jax.ShapeDtypeStruct((bands, n_e, rows * LANES), jnp.float32),
        scratch_shapes=[pltpu.VMEM((n_e, bands * rows, LANES), jnp.float32)],
        compiler_params=params(),
        cost_estimate=cost(bands * n_e * rows * LANES, bands * n_e * rows * LANES * 8),
        name="place_coadd",
    )(*pieces)


def place_morph(pieces, bands):
    n_e = len(pieces)
    slots, lanes = pieces[0].shape
    lanes -= LANES

    def kernel(*refs):
        ins, out, spec, scr = refs[:n_e], refs[n_e], refs[n_e + 1], refs[n_e + 2]
        e = lax.axis_index("epoch")
        for p in range(n_e):
            q = jnp.bitwise_xor(e, p)
            out[q] = ins[p][:, 0:lanes]
            scr[q] = ins[p][:, lanes : lanes + LANES]
        for c in range(bands):
            for q in range(n_e):
                spec[c, q : q + 1, :] = scr[q, pl.ds(c, 1), 0:slots]

    return pl.pallas_call(
        kernel,
        in_specs=[whole()] * n_e,
        out_specs=[whole()] * 2,
        out_shape=[
            jax.ShapeDtypeStruct((n_e, slots, lanes), jnp.float32),
            jax.ShapeDtypeStruct((bands, n_e, slots), jnp.float32),
        ],
        scratch_shapes=[pltpu.VMEM((n_e, slots, LANES), jnp.float32)],
        compiler_params=params(),
        cost_estimate=cost(n_e * slots * lanes, n_e * slots * lanes * 8),
        name="place_morph",
    )(*pieces)


def xor_permute(x, axis, size, mask):
    return lax.ppermute(x, axis, [(i, i ^ mask) for i in range(size)])


def on_device_blend(
    n_e, n_b, visit_flux, visit_precision, visit_live, footprint, source_count, spectra_init, morphology_init
):
    owned, slots, _ = morphology_init.shape
    bands = visit_flux.shape[2]
    cores = 2
    e = lax.axis_index("epoch")
    flux = hbm(jnp.transpose(visit_flux, (0, 2, 1, 3)))
    prec = hbm(jnp.transpose(visit_precision, (0, 2, 1, 3)))

    def swap(xs):
        out = [xs[0]]
        for p in range(1, n_e):
            out.append(xor_permute(xs[p], "epoch", n_e, p))
        return out

    spectra = lax.dynamic_index_in_dim(spectra_init, e, 0, keepdims=False)
    spectra = jnp.transpose(spectra).reshape(bands * slots, 1)
    spectra = jnp.broadcast_to(spectra, (bands * slots, LANES))

    chips = n_b // cores
    chunks = [[k] for k in range(chips - 1, 1, -1)] + [[1, 0] if chips > 1 else [0]]
    pieces = [None] * n_b
    for ks in chunks:
        s0, k0, s1, k1 = visit_sums(flux, prec, visit_live, ks, owned, n_e, cores)
        for d, (send, keep, first, second) in enumerate(((s0, k0, 1, 2), (s1, k1, 2, 1))):
            got = xor_permute(send, "epoch", n_e, first)
            onward = xor_permute(keep[1] + got[1], "epoch", n_e, second)
            full = keep[0] + got[0] + onward
            for i, k in enumerate(ks):
                m = k * cores + d
                pieces[m] = xor_permute(full[i], "blend", n_b, m) if m else full[i]
    packed = pack_kernel(hbm(morphology_init), hbm(footprint), n_e)
    packed = swap(packed)
    cov, *coadds = coadd_kernel(pieces, bands, n_e)
    blocks = deblend_kernel(source_count, cov, coadds, packed, spectra)
    out_coadd = place_coadd(swap(coadds))
    out_morph, out_spec = place_morph(swap(blocks), bands)
    return (jnp.transpose(out_coadd, (1, 0, 2)), jnp.transpose(out_spec, (1, 2, 0)), out_morph)


def solution(mesh):
    n_e, n_b = mesh.shape["epoch"], mesh.shape["blend"]
    in_specs = (
        P("epoch", None, None, "blend"),
        P("epoch", None, None, "blend"),
        P("epoch", None),
        P("blend", None, "epoch"),
        P("blend"),
        P("blend", None, None),
        P("blend", None, "epoch"),
    )
    out_specs = (P("blend", None, "epoch"), P("blend", None, None), P("blend", None, "epoch"))

    def on_device(*args):
        owned, slots, pix_part = args[6].shape
        pix = args[0].shape[3]
        by_blend = (
            n_e == 4
            and owned == n_e
            and slots == 8
            and n_b % 2 == 0
            and n_b & (n_b - 1) == 0
            and pix % (8 * LANES) == 0
            and pix_part % pix == 0
            and pix_part % (8 * LANES) == 0
        )
        if by_blend:
            return on_device_blend(n_e, n_b, *args)
        return on_device_general(*args)

    return jax.shard_map(
        on_device, mesh=mesh, in_specs=in_specs, out_specs=out_specs, check_vma=False
    )
```

```python
import jax
import jax.numpy as jnp
from jax import lax
from jax.experimental import pallas as pl
from jax.experimental.pallas import tpu as pltpu
from jax.sharding import PartitionSpec as P


ITERS = 2
LANES = 128


def on_device_general(
    visit_flux, visit_precision, visit_live, footprint, source_count, spectra_init, morphology_init
):
    weights = visit_precision.astype(jnp.float32) * visit_live.astype(jnp.float32)[:, :, None, None]
    numerator = jnp.sum(weights * visit_flux.astype(jnp.float32), axis=0)
    weight_sum = jnp.sum(weights, axis=0)
    pix_part = morphology_init.shape[2]
    owned = morphology_init.shape[0]
    numerator, weight_sum = (
        lax.psum_scatter(numerator, "epoch", scatter_dimension=2, tiled=True),
        lax.psum_scatter(weight_sum, "epoch", scatter_dimension=2, tiled=True),
    )
    every_blend, band_count, piece = numerator.shape
    numerator = numerator.reshape(every_blend, band_count, 1, piece)
    weight_sum = weight_sum.reshape(every_blend, band_count, 1, piece)
    numerator, weight_sum = (
        lax.all_to_all(numerator, "blend", split_axis=0, concat_axis=2, tiled=True),
        lax.all_to_all(weight_sum, "blend", split_axis=0, concat_axis=2, tiled=True),
    )
    blocks = numerator.shape[2]
    numerator = numerator.reshape(owned, band_count, blocks, 1, piece)
    weight_sum = weight_sum.reshape(owned, band_count, blocks, 1, piece)
    numerator, weight_sum = (
        lax.all_to_all(numerator, "epoch", split_axis=2, concat_axis=3, tiled=True),
        lax.all_to_all(weight_sum, "epoch", split_axis=2, concat_axis=3, tiled=True),
    )
    numerator = numerator.reshape(owned, band_count, pix_part)
    weight_sum = weight_sum.reshape(owned, band_count, pix_part)
    coadd_flux = numerator / (1.0 + weight_sum)
    coverage = weight_sum / (1.0 + weight_sum)
    slots = footprint.shape[1]
    source_live = (jnp.arange(slots, dtype=jnp.int32)[None, :] < source_count[:, None]).astype(
        jnp.float32
    )
    footprint_mask = footprint.astype(jnp.float32) * source_live[:, :, None]
    live_count = source_count.astype(jnp.float32)
    morphology = morphology_init * footprint_mask
    spectra = spectra_init
    highest = lax.Precision.HIGHEST
    for _ in range(ITERS):
        blend_model = jnp.einsum("bkc,bkp->bcp", spectra, morphology, precision=highest)
        residual = coverage * (coadd_flux - blend_model)
        morph_grad = jnp.einsum("bkc,bcp->bkp", spectra, residual, precision=highest)
        morph_step = 1.0 / (1.0 + live_count[:, None] * jnp.sum(spectra * spectra, axis=2))
        morphology = (
            jnp.maximum(0.0, morphology + morph_grad * morph_step[:, :, None]) * footprint_mask
        )
        blend_model = jnp.einsum("bkc,bkp->bcp", spectra, morphology, precision=highest)
        residual = coverage * (coadd_flux - blend_model)
        spectra_grad = jnp.einsum("bkp,bcp->bkc", morphology, residual, precision=highest)
        morph_norm = jnp.sum(morphology * morphology, axis=2)
        spectra_grad, morph_norm = lax.psum((spectra_grad, morph_norm), "epoch")
        spectra = jnp.maximum(
            0.0, spectra + spectra_grad / (1.0 + live_count[:, None] * morph_norm)[:, :, None]
        )
    return (coadd_flux, spectra, morphology)


VMEM_LIMIT = 6 * 1024 * 1024
SMALL_LIMIT = 1024 * 1024


def hbm(x):
    return pltpu.with_memory_space_constraint(x, pltpu.HBM)


def vmem(x):
    return pltpu.with_memory_space_constraint(x, pltpu.VMEM)


def whole():
    return pl.BlockSpec(memory_space=pltpu.VMEM)


def in_place():
    return pl.BlockSpec(memory_space=pltpu.HBM)


def cost(flops, nbytes):
    return pl.CostEstimate(flops=int(flops), bytes_accessed=int(nbytes), transcendentals=0)


def params(limit=VMEM_LIMIT):
    return pltpu.CompilerParams(vmem_limit_bytes=limit)


def visit_sums(flux, prec, live, ks, owned, n_e, cores, fetched):
    epochs, bands, blends, pix = flux.shape
    group = cores * owned
    rows = pix // LANES
    block_rows = 2 * bands * rows
    half = n_e // 2
    n_k = len(ks)
    order = {0: ((1, 3), (0, 2)), 1: ((2, 3), (0, 1))}

    def kernel(live_in, flux_in, prec_in, s0, k0, s1, k1, scr, *own):
        e, b = lax.axis_index("epoch"), lax.axis_index("blend")
        chip, c = b // cores, b % cores

        def at_rows(i):
            return pl.ds(pl.multiple_of((chip ^ ks[i]) * group, 8), group)

        if fetched:
            live_ref = live_in

            def load(ref, i, band, ep, at):
                return ref[ep, band, at_rows(i), at].astype(jnp.float32)

            refs = (flux_in, prec_in)
        else:
            fbuf, pbuf, live_ref, sems, live_sem = own

            def copies(i, band):
                return [
                    pltpu.make_async_copy(ref.at[:, band, at_rows(i), :], buf.at[i, band], sems.at[i, band, n])
                    for n, (ref, buf) in enumerate(((flux_in, fbuf), (prec_in, pbuf)))
                ]

            live_copy = pltpu.make_async_copy(live_in, live_ref, live_sem)
            live_copy.start()
            for i in range(n_k):
                for band in range(bands):
                    for copy in copies(i, band):
                        copy.start()
            live_copy.wait()

            def load(ref, i, band, ep, at):
                return ref[i, band, ep, :, at].astype(jnp.float32)

            refs = (fbuf, pbuf)
        sub = lax.broadcasted_iota(jnp.int32, (group, blends), 0)
        lane = lax.broadcasted_iota(jnp.int32, (group, blends), 1)
        for i in range(n_k):
            pick = lane == sub + (chip ^ ks[i]) * group
            lives = []
            for ep in range(epochs):
                row = live_ref[ep : ep + 1, :].astype(jnp.float32)
                col = jnp.where(pick, jnp.broadcast_to(row, pick.shape), 0.0)
                lives.append(jnp.broadcast_to(jnp.sum(col, axis=1, keepdims=True), (group, LANES)))
            for band in range(bands):
                if not fetched:
                    for copy in copies(i, band):
                        copy.wait()
                for j in range(rows):
                    at = pl.ds(j * LANES, LANES)
                    num = wsum = None
                    for ep in range(epochs):
                        w = load(refs[1], i, band, ep, at) * lives[ep]
                        n = w * load(refs[0], i, band, ep, at)
                        num = n if num is None else num + n
                        wsum = w if wsum is None else wsum + w
                    scr[pl.ds(band * rows + j, group, stride=block_rows), :] = num
                    scr[pl.ds((bands + band) * rows + j, group, stride=block_rows), :] = wsum
            for d, outs in ((0, (s0, k0)), (1, (s1, k1))):
                for ref, slots in zip(outs, order[d]):
                    for slot, p in enumerate(slots):
                        r = jnp.bitwise_xor(c, d) * n_e + jnp.bitwise_xor(e, p)
                        start = pl.multiple_of(r * block_rows, 8)
                        ref[slot, i] = scr[pl.ds(start, block_rows), :].reshape(2 * bands, rows, LANES)

    scratch = [pltpu.VMEM((group * block_rows, LANES), jnp.float32)]
    if not fetched:
        scratch += [
            pltpu.VMEM((n_k, bands, epochs, group, pix), flux.dtype),
            pltpu.VMEM((n_k, bands, epochs, group, pix), prec.dtype),
            pltpu.VMEM(live.shape, live.dtype),
            pltpu.SemaphoreType.DMA((n_k, bands, 2)),
            pltpu.SemaphoreType.DMA,
        ]
    out = pltpu.VMEM((half, n_k, 2 * bands, rows, LANES), jnp.float32)
    n_in = n_k * epochs * bands * group * pix
    put = vmem if fetched else hbm
    return pl.pallas_call(
        kernel,
        in_specs=[whole() if fetched else in_place()] * 3,
        out_specs=[whole()] * 4,
        out_shape=[out] * 4,
        scratch_shapes=scratch,
        compiler_params=params(),
        cost_estimate=cost(n_in * 6, n_in * 4 + n_in * 2),
        name="visit_sums",
    )(put(live), put(flux), put(prec))


def halve_kernel(keep, got):
    def kernel(keep_ref, got_ref, part, onward):
        part[...] = keep_ref[0] + got_ref[0]
        onward[...] = keep_ref[1] + got_ref[1]

    out = pltpu.VMEM(keep.shape[1:], keep.dtype)
    return pl.pallas_call(
        kernel,
        in_specs=[whole()] * 2,
        out_specs=[whole()] * 2,
        out_shape=[out] * 2,
        compiler_params=params(SMALL_LIMIT),
        cost_estimate=cost(keep.size, keep.size * 12),
        name="halve",
    )(keep, vmem(got))


def finish_kernel(part, got):
    n_k = part.shape[0]

    def kernel(part_ref, got_ref, *outs):
        for i in range(n_k):
            outs[i][...] = part_ref[i] + got_ref[i]

    return pl.pallas_call(
        kernel,
        in_specs=[whole()] * 2,
        out_specs=[whole()] * n_k,
        out_shape=[pltpu.VMEM(part.shape[1:], part.dtype)] * n_k,
        compiler_params=params(SMALL_LIMIT),
        cost_estimate=cost(part.size, part.size * 12),
        name="finish",
    )(part, vmem(got))


def pack_kernel(morph, footprint, n_e):
    _, slots, lanes = morph.shape

    def kernel(morph_ref, foot_ref, *refs):
        outs, buf, sems = refs[:n_e], refs[n_e], refs[n_e + 1]
        e = lax.axis_index("epoch")
        copies = []
        for p in range(n_e):
            q = jnp.bitwise_xor(e, p)
            copies.append(
                (
                    pltpu.make_async_copy(morph_ref.at[q], outs[p].at[0], sems.at[p, 0]),
                    pltpu.make_async_copy(foot_ref.at[q], buf.at[p], sems.at[p, 1]),
                )
            )
        for pair in copies:
            for copy in pair:
                copy.start()
        for p, pair in enumerate(copies):
            for copy in pair:
                copy.wait()
            outs[p][1] = buf[p].astype(jnp.float32)

    n = n_e * slots * lanes
    return pl.pallas_call(
        kernel,
        in_specs=[in_place()] * 2,
        out_specs=[whole()] * n_e,
        out_shape=[pltpu.VMEM((2, slots, lanes), jnp.float32)] * n_e,
        scratch_shapes=[
            pltpu.VMEM((n_e, slots, lanes), footprint.dtype),
            pltpu.SemaphoreType.DMA((n_e, 2)),
        ],
        compiler_params=params(),
        cost_estimate=cost(n * 2, n * 16),
        name="pack",
    )(morph, footprint)


def coadd_kernel(pieces, bands, n_e):
    n_b = len(pieces)
    rows = pieces[0].shape[1]
    total = n_b * rows
    per_e = total // n_e

    def kernel(*refs):
        ins, cov, outs, scr = refs[:n_b], refs[n_b], refs[n_b + 1 : n_b + 1 + n_e], refs[-1]
        e, b = lax.axis_index("epoch"), lax.axis_index("blend")
        for m in range(n_b):
            start = pl.multiple_of(jnp.bitwise_xor(b, m) * rows, 8)
            for band in range(bands):
                num, wsum = ins[m][band], ins[m][bands + band]
                inv = 1.0 / (1.0 + wsum)
                cov[band, pl.ds(start, rows), :] = wsum * inv
                scr[band, pl.ds(start, rows), :] = num * inv
        for p in range(n_e):
            start = pl.multiple_of(jnp.bitwise_xor(e, p) * per_e, 8)
            for band in range(bands):
                outs[p][band] = scr[band, pl.ds(start, per_e), :]

    return pl.pallas_call(
        kernel,
        in_specs=[whole()] * n_b,
        out_specs=[whole()] * (1 + n_e),
        out_shape=[jax.ShapeDtypeStruct((bands, total, LANES), jnp.float32)]
        + [jax.ShapeDtypeStruct((bands, per_e, LANES), jnp.float32)] * n_e,
        scratch_shapes=[pltpu.VMEM((bands, total, LANES), jnp.float32)],
        compiler_params=params(),
        cost_estimate=cost(bands * total * LANES * 8, bands * total * LANES * 16),
        name="coadd",
    )(*pieces)


def deblend_kernel(counts, cov, coadds, packed, spectra):
    n_e = len(coadds)
    bands, total, _ = cov.shape
    _, slots, lanes = packed[0].shape
    per_e = lanes // LANES
    groups = total // 8

    def kernel(count_ref, cov_ref, *refs):
        co_in, pk_in = refs[:n_e], refs[n_e : 2 * n_e]
        spec_ref = refs[2 * n_e]
        outs = refs[2 * n_e + 1 : 3 * n_e + 1]
        co, mo, ma, res, acc, spec, step = refs[3 * n_e + 1 :]
        e = lax.axis_index("epoch")
        count = count_ref[e]
        n_live = count.astype(jnp.float32)
        k_iota = lax.broadcasted_iota(jnp.int32, (slots, LANES), 0)
        live = (k_iota < count).astype(jnp.float32)
        for p in range(n_e):
            start = jnp.bitwise_xor(e, p) * per_e
            for band in range(bands):
                co[band, pl.ds(pl.multiple_of(start, 8), per_e), :] = co_in[p][band]
            for j in range(per_e):
                at = pl.ds(j * LANES, LANES)
                mask = pk_in[p][1, :, at] * live
                ma[pl.ds(start + j, slots, stride=total), :] = mask
                mo[pl.ds(start + j, slots, stride=total), :] = pk_in[p][0, :, at] * mask
        lane = lax.broadcasted_iota(jnp.int32, (slots, LANES), 1)
        small = (slots, spec_ref.shape[2])
        diag = lax.broadcasted_iota(jnp.int32, small, 0) == lax.broadcasted_iota(jnp.int32, small, 1)
        for c in range(bands):
            row = jnp.broadcast_to(spec_ref[c, pl.ds(e, 1), :], small)
            col = jnp.sum(jnp.where(diag, row, 0.0), axis=1, keepdims=True)
            spec[pl.ds(c * slots, slots), :] = jnp.broadcast_to(col, (slots, LANES))

        def bcast(ref, row):
            return jnp.broadcast_to(ref[pl.ds(row, 1), :], (8, LANES))

        for _ in range(ITERS):
            square = None
            for band in range(bands):
                s = spec[pl.ds(band * slots, slots), :]
                square = s * s if square is None else square + s * s
            step[...] = 1.0 / (1.0 + n_live * square)

            def group(g, carry):
                at = pl.multiple_of(g * 8, 8)
                m = [mo[pl.ds(pl.multiple_of(k * total + at, 8), 8), :] for k in range(slots)]
                cv = [cov_ref[c, pl.ds(at, 8), :] for c in range(bands)]
                cd = [co[c, pl.ds(at, 8), :] for c in range(bands)]
                r = []
                for c in range(bands):
                    model = None
                    for k in range(slots):
                        t = bcast(spec, c * slots + k) * m[k]
                        model = t if model is None else model + t
                    r.append(cv[c] * (cd[c] - model))
                for k in range(slots):
                    grad = None
                    for c in range(bands):
                        t = bcast(spec, c * slots + k) * r[c]
                        grad = t if grad is None else grad + t
                    mk = ma[pl.ds(pl.multiple_of(k * total + at, 8), 8), :]
                    m[k] = jnp.maximum(0.0, m[k] + grad * bcast(step, k)) * mk
                    mo[pl.ds(pl.multiple_of(k * total + at, 8), 8), :] = m[k]
                for c in range(bands):
                    model = None
                    for k in range(slots):
                        t = bcast(spec, c * slots + k) * m[k]
                        model = t if model is None else model + t
                    res[c, pl.ds(at, 8), :] = cv[c] * (cd[c] - model)
                return carry

            lax.fori_loop(0, groups, group, 0, unroll=2)
            for k in range(slots):
                sums = [None] * (bands + 1)
                for g in range(groups):
                    m = mo[pl.ds(k * total + g * 8, 8), :]
                    for c in range(bands):
                        t = m * res[c, pl.ds(g * 8, 8), :]
                        sums[c] = t if sums[c] is None else sums[c] + t
                    t = m * m
                    sums[bands] = t if sums[bands] is None else sums[bands] + t
                for c in range(bands + 1):
                    acc[pl.ds((c * slots + k) * 8, 8), :] = sums[c]

            def reduced(c):
                v = None
                for s in range(8):
                    t = acc[pl.ds(c * slots * 8 + s, slots, stride=8), :]
                    v = t if v is None else v + t
                return jnp.broadcast_to(jnp.sum(v, axis=1, keepdims=True), (slots, LANES))

            den = 1.0 + n_live * reduced(bands)
            for c in range(bands):
                s = spec[pl.ds(c * slots, slots), :]
                spec[pl.ds(c * slots, slots), :] = jnp.maximum(0.0, s + reduced(c) / den)

        tile = jnp.zeros((slots, LANES), jnp.float32)
        for c in range(bands):
            on_diag = jnp.where(lane == k_iota, spec[pl.ds(c * slots, slots), :], 0.0)
            row = jnp.broadcast_to(jnp.sum(on_diag, axis=0, keepdims=True), (slots, LANES))
            tile = jnp.where(k_iota == c, row, tile)
        for p in range(n_e):
            start = jnp.bitwise_xor(e, p) * per_e
            for j in range(per_e):
                outs[p][:, pl.ds(j * LANES, LANES)] = mo[pl.ds(start + j, slots, stride=total), :]
            outs[p][:, pl.ds(lanes, LANES)] = tile

    f32 = jnp.float32
    return pl.pallas_call(
        kernel,
        in_specs=[pl.BlockSpec(memory_space=pltpu.SMEM)] + [whole()] * (2 * n_e + 2),
        out_specs=[whole()] * n_e,
        out_shape=[jax.ShapeDtypeStruct((slots, lanes + LANES), f32)] * n_e,
        scratch_shapes=[
            pltpu.VMEM((bands, total, LANES), f32),
            pltpu.VMEM((slots * total, LANES), f32),
            pltpu.VMEM((slots * total, LANES), f32),
            pltpu.VMEM((bands, total, LANES), f32),
            pltpu.VMEM(((bands + 1) * slots * 8, LANES), f32),
            pltpu.VMEM((bands * slots, LANES), f32),
            pltpu.VMEM((slots, LANES), f32),
        ],
        compiler_params=params(),
        cost_estimate=cost(total * LANES * slots * bands * 8 * ITERS, total * LANES * 4 * 30),
        name="deblend",
    )(counts, cov, *coadds, *packed, spectra)


def place_coadd(pieces):
    n_e = len(pieces)
    bands, rows, _ = pieces[0].shape

    def kernel(*refs):
        ins, out, scr = refs[:n_e], refs[n_e], refs[n_e + 1]
        e = lax.axis_index("epoch")
        for p in range(n_e):
            scr[jnp.bitwise_xor(e, p)] = ins[p][...].reshape(bands * rows, LANES)
        for band in range(bands):
            for j in range(rows):
                for q in range(n_e):
                    out[band, q : q + 1, pl.ds(j * LANES, LANES)] = scr[q, pl.ds(band * rows + j, 1), :]

    return pl.pallas_call(
        kernel,
        in_specs=[whole()] * n_e,
        out_specs=whole(),
        out_shape=jax.ShapeDtypeStruct((bands, n_e, rows * LANES), jnp.float32),
        scratch_shapes=[pltpu.VMEM((n_e, bands * rows, LANES), jnp.float32)],
        compiler_params=params(),
        cost_estimate=cost(bands * n_e * rows * LANES, bands * n_e * rows * LANES * 8),
        name="place_coadd",
    )(*pieces)


def place_morph(pieces, bands):
    n_e = len(pieces)
    slots, lanes = pieces[0].shape
    lanes -= LANES

    def kernel(*refs):
        ins, out, spec, scr = refs[:n_e], refs[n_e], refs[n_e + 1], refs[n_e + 2]
        e = lax.axis_index("epoch")
        for p in range(n_e):
            q = jnp.bitwise_xor(e, p)
            out[q] = ins[p][:, 0:lanes]
            scr[q] = ins[p][:, lanes : lanes + LANES]
        for c in range(bands):
            for q in range(n_e):
                spec[c, q : q + 1, :] = scr[q, pl.ds(c, 1), 0:slots]

    return pl.pallas_call(
        kernel,
        in_specs=[whole()] * n_e,
        out_specs=[whole()] * 2,
        out_shape=[
            jax.ShapeDtypeStruct((n_e, slots, lanes), jnp.float32),
            jax.ShapeDtypeStruct((bands, n_e, slots), jnp.float32),
        ],
        scratch_shapes=[pltpu.VMEM((n_e, slots, LANES), jnp.float32)],
        compiler_params=params(),
        cost_estimate=cost(n_e * slots * lanes, n_e * slots * lanes * 8),
        name="place_morph",
    )(*pieces)


def xor_permute(x, axis, size, mask):
    return lax.ppermute(x, axis, [(i, i ^ mask) for i in range(size)])


def on_device_blend(
    n_e, n_b, visit_flux, visit_precision, visit_live, footprint, source_count, spectra_init, morphology_init
):
    owned, _, _ = morphology_init.shape
    bands = visit_flux.shape[2]
    cores = 2
    flux = jnp.transpose(visit_flux, (0, 2, 1, 3))
    prec = jnp.transpose(visit_precision, (0, 2, 1, 3))


    def swap(xs):
        out = [xs[0]]
        for p in range(1, n_e):
            out.append(xor_permute(xs[p], "epoch", n_e, p))
        return out

    spectra = jnp.transpose(spectra_init, (2, 0, 1))

    chips = n_b // cores
    chunks = [[k] for k in range(chips - 1, 1, -1)] + [[1, 0] if chips > 1 else [0]]
    pieces = [None] * n_b
    for n, ks in enumerate(chunks):
        s0, k0, s1, k1 = visit_sums(flux, prec, visit_live, ks, owned, n_e, cores, n > 0)
        for d, (send, keep, first, second) in enumerate(((s0, k0, 1, 2), (s1, k1, 2, 1))):
            got = xor_permute(send, "epoch", n_e, first)
            part, onward = halve_kernel(keep, got)
            got = xor_permute(onward, "epoch", n_e, second)
            full = finish_kernel(part, got)
            for i, k in enumerate(ks):
                m = k * cores + d
                pieces[m] = xor_permute(full[i], "blend", n_b, m) if m else full[i]
    packed = pack_kernel(hbm(morphology_init), hbm(footprint), n_e)
    packed = swap(packed)
    cov, *coadds = coadd_kernel(pieces, bands, n_e)
    blocks = deblend_kernel(source_count, cov, coadds, packed, spectra)
    out_coadd = place_coadd(swap(coadds))
    out_morph, out_spec = place_morph(swap(blocks), bands)
    return (jnp.transpose(out_coadd, (1, 0, 2)), jnp.transpose(out_spec, (1, 2, 0)), out_morph)


def solution(mesh):
    n_e, n_b = mesh.shape["epoch"], mesh.shape["blend"]
    in_specs = (
        P("epoch", None, None, "blend"),
        P("epoch", None, None, "blend"),
        P("epoch", None),
        P("blend", None, "epoch"),
        P("blend"),
        P("blend", None, None),
        P("blend", None, "epoch"),
    )
    out_specs = (P("blend", None, "epoch"), P("blend", None, None), P("blend", None, "epoch"))

    def on_device(*args):
        owned, slots, pix_part = args[6].shape
        pix = args[0].shape[3]
        by_blend = (
            n_e == 4
            and owned == n_e
            and slots == 8
            and n_b % 2 == 0
            and n_b & (n_b - 1) == 0
            and pix % (8 * LANES) == 0
            and pix_part % pix == 0
            and pix_part % (8 * LANES) == 0
        )
        if by_blend:
            return on_device_blend(n_e, n_b, *args)
        return on_device_general(*args)

    return jax.shard_map(
        on_device, mesh=mesh, in_specs=in_specs, out_specs=out_specs, check_vma=False
    )
```

```python
import jax
import jax.numpy as jnp
from jax import lax
from jax.experimental import pallas as pl
from jax.experimental.pallas import tpu as pltpu
from jax.sharding import PartitionSpec as P


ITERS = 2
LANES = 128


def on_device_general(
    visit_flux, visit_precision, visit_live, footprint, source_count, spectra_init, morphology_init
):
    weights = visit_precision.astype(jnp.float32) * visit_live.astype(jnp.float32)[:, :, None, None]
    numerator = jnp.sum(weights * visit_flux.astype(jnp.float32), axis=0)
    weight_sum = jnp.sum(weights, axis=0)
    pix_part = morphology_init.shape[2]
    owned = morphology_init.shape[0]
    numerator, weight_sum = (
        lax.psum_scatter(numerator, "epoch", scatter_dimension=2, tiled=True),
        lax.psum_scatter(weight_sum, "epoch", scatter_dimension=2, tiled=True),
    )
    every_blend, band_count, piece = numerator.shape
    numerator = numerator.reshape(every_blend, band_count, 1, piece)
    weight_sum = weight_sum.reshape(every_blend, band_count, 1, piece)
    numerator, weight_sum = (
        lax.all_to_all(numerator, "blend", split_axis=0, concat_axis=2, tiled=True),
        lax.all_to_all(weight_sum, "blend", split_axis=0, concat_axis=2, tiled=True),
    )
    blocks = numerator.shape[2]
    numerator = numerator.reshape(owned, band_count, blocks, 1, piece)
    weight_sum = weight_sum.reshape(owned, band_count, blocks, 1, piece)
    numerator, weight_sum = (
        lax.all_to_all(numerator, "epoch", split_axis=2, concat_axis=3, tiled=True),
        lax.all_to_all(weight_sum, "epoch", split_axis=2, concat_axis=3, tiled=True),
    )
    numerator = numerator.reshape(owned, band_count, pix_part)
    weight_sum = weight_sum.reshape(owned, band_count, pix_part)
    coadd_flux = numerator / (1.0 + weight_sum)
    coverage = weight_sum / (1.0 + weight_sum)
    slots = footprint.shape[1]
    source_live = (jnp.arange(slots, dtype=jnp.int32)[None, :] < source_count[:, None]).astype(
        jnp.float32
    )
    footprint_mask = footprint.astype(jnp.float32) * source_live[:, :, None]
    live_count = source_count.astype(jnp.float32)
    morphology = morphology_init * footprint_mask
    spectra = spectra_init
    highest = lax.Precision.HIGHEST
    for _ in range(ITERS):
        blend_model = jnp.einsum("bkc,bkp->bcp", spectra, morphology, precision=highest)
        residual = coverage * (coadd_flux - blend_model)
        morph_grad = jnp.einsum("bkc,bcp->bkp", spectra, residual, precision=highest)
        morph_step = 1.0 / (1.0 + live_count[:, None] * jnp.sum(spectra * spectra, axis=2))
        morphology = (
            jnp.maximum(0.0, morphology + morph_grad * morph_step[:, :, None]) * footprint_mask
        )
        blend_model = jnp.einsum("bkc,bkp->bcp", spectra, morphology, precision=highest)
        residual = coverage * (coadd_flux - blend_model)
        spectra_grad = jnp.einsum("bkp,bcp->bkc", morphology, residual, precision=highest)
        morph_norm = jnp.sum(morphology * morphology, axis=2)
        spectra_grad, morph_norm = lax.psum((spectra_grad, morph_norm), "epoch")
        spectra = jnp.maximum(
            0.0, spectra + spectra_grad / (1.0 + live_count[:, None] * morph_norm)[:, :, None]
        )
    return (coadd_flux, spectra, morphology)


VMEM_LIMIT = 6 * 1024 * 1024
SMALL_LIMIT = 1024 * 1024


def hbm(x):
    return pltpu.with_memory_space_constraint(x, pltpu.HBM)


def vmem(x):
    return pltpu.with_memory_space_constraint(x, pltpu.VMEM)


def whole():
    return pl.BlockSpec(memory_space=pltpu.VMEM)


def in_place():
    return pl.BlockSpec(memory_space=pltpu.HBM)


def cost(flops, nbytes):
    return pl.CostEstimate(flops=int(flops), bytes_accessed=int(nbytes), transcendentals=0)


def params(limit=VMEM_LIMIT):
    return pltpu.CompilerParams(vmem_limit_bytes=limit)


def visit_sums(flux, prec, live, ks, owned, n_e, cores, fetched):
    epochs, bands, blends, pix = flux.shape
    group = cores * owned
    rows = pix // LANES
    block_rows = 2 * bands * rows
    half = n_e // 2
    n_k = len(ks)
    order = {0: ((1, 3), (0, 2)), 1: ((2, 3), (0, 1))}

    def kernel(live_in, flux_in, prec_in, s0, k0, s1, k1, scr, *own):
        e, b = lax.axis_index("epoch"), lax.axis_index("blend")
        chip, c = b // cores, b % cores

        def at_rows(i):
            return pl.ds(pl.multiple_of((chip ^ ks[i]) * group, 8), group)

        if fetched:
            live_ref = live_in

            def load(ref, i, band, ep, at):
                return ref[ep, band, at_rows(i), at].astype(jnp.float32)

            refs = (flux_in, prec_in)
        else:
            fbuf, pbuf, live_ref, sems, live_sem = own

            def copies(i, band):
                return [
                    pltpu.make_async_copy(ref.at[:, band, at_rows(i), :], buf.at[i, band], sems.at[i, band, n])
                    for n, (ref, buf) in enumerate(((flux_in, fbuf), (prec_in, pbuf)))
                ]

            live_copy = pltpu.make_async_copy(live_in, live_ref, live_sem)
            live_copy.start()
            for i in range(n_k):
                for band in range(bands):
                    for copy in copies(i, band):
                        copy.start()
            live_copy.wait()

            def load(ref, i, band, ep, at):
                return ref[i, band, ep, :, at].astype(jnp.float32)

            refs = (fbuf, pbuf)
        sub = lax.broadcasted_iota(jnp.int32, (group, blends), 0)
        lane = lax.broadcasted_iota(jnp.int32, (group, blends), 1)
        for i in range(n_k):
            pick = lane == sub + (chip ^ ks[i]) * group
            lives = []
            for ep in range(epochs):
                row = live_ref[ep : ep + 1, :].astype(jnp.float32)
                col = jnp.where(pick, jnp.broadcast_to(row, pick.shape), 0.0)
                lives.append(jnp.broadcast_to(jnp.sum(col, axis=1, keepdims=True), (group, LANES)))
            for band in range(bands):
                if not fetched:
                    for copy in copies(i, band):
                        copy.wait()
                for j in range(rows):
                    at = pl.ds(j * LANES, LANES)
                    num = wsum = None
                    for ep in range(epochs):
                        w = load(refs[1], i, band, ep, at) * lives[ep]
                        n = w * load(refs[0], i, band, ep, at)
                        num = n if num is None else num + n
                        wsum = w if wsum is None else wsum + w
                    scr[pl.ds(band * rows + j, group, stride=block_rows), :] = num
                    scr[pl.ds((bands + band) * rows + j, group, stride=block_rows), :] = wsum
            for d, outs in ((0, (s0, k0)), (1, (s1, k1))):
                for ref, slots in zip(outs, order[d]):
                    for slot, p in enumerate(slots):
                        r = jnp.bitwise_xor(c, d) * n_e + jnp.bitwise_xor(e, p)
                        start = pl.multiple_of(r * block_rows, 8)
                        ref[slot, i] = scr[pl.ds(start, block_rows), :].reshape(2 * bands, rows, LANES)

    scratch = [pltpu.VMEM((group * block_rows, LANES), jnp.float32)]
    if not fetched:
        scratch += [
            pltpu.VMEM((n_k, bands, epochs, group, pix), flux.dtype),
            pltpu.VMEM((n_k, bands, epochs, group, pix), prec.dtype),
            pltpu.VMEM(live.shape, live.dtype),
            pltpu.SemaphoreType.DMA((n_k, bands, 2)),
            pltpu.SemaphoreType.DMA,
        ]
    out = pltpu.VMEM((half, n_k, 2 * bands, rows, LANES), jnp.float32)
    n_in = n_k * epochs * bands * group * pix
    put = vmem if fetched else hbm
    return pl.pallas_call(
        kernel,
        in_specs=[whole() if fetched else in_place()] * 3,
        out_specs=[whole()] * 4,
        out_shape=[out] * 4,
        scratch_shapes=scratch,
        compiler_params=params(),
        cost_estimate=cost(n_in * 6, n_in * 4 + n_in * 2),
        name="visit_sums",
    )(put(live), put(flux), put(prec))


def halve_kernel(keep, got):
    def kernel(keep_ref, got_ref, part, onward):
        part[...] = keep_ref[0] + got_ref[0]
        onward[...] = keep_ref[1] + got_ref[1]

    out = pltpu.VMEM(keep.shape[1:], keep.dtype)
    return pl.pallas_call(
        kernel,
        in_specs=[whole()] * 2,
        out_specs=[whole()] * 2,
        out_shape=[out] * 2,
        compiler_params=params(SMALL_LIMIT),
        cost_estimate=cost(keep.size, keep.size * 12),
        name="halve",
    )(keep, vmem(got))


def finish_kernel(part, got):
    n_k = part.shape[0]

    def kernel(part_ref, got_ref, *outs):
        for i in range(n_k):
            outs[i][...] = part_ref[i] + got_ref[i]

    return pl.pallas_call(
        kernel,
        in_specs=[whole()] * 2,
        out_specs=[whole()] * n_k,
        out_shape=[pltpu.VMEM(part.shape[1:], part.dtype)] * n_k,
        compiler_params=params(SMALL_LIMIT),
        cost_estimate=cost(part.size, part.size * 12),
        name="finish",
    )(part, vmem(got))


def pack_kernel(counts, morph, footprint, n_e):
    _, slots, lanes = morph.shape
    rows = lanes // LANES

    def kernel(count_ref, morph_ref, foot_ref, *refs):
        outs, mbuf, fbuf, sems = refs[:n_e], refs[n_e], refs[n_e + 1], refs[n_e + 2]
        e = lax.axis_index("epoch")
        copies = []
        for p in range(n_e):
            q = jnp.bitwise_xor(e, p)
            copies.append(
                (
                    pltpu.make_async_copy(morph_ref.at[q], mbuf.at[p], sems.at[p, 0]),
                    pltpu.make_async_copy(foot_ref.at[q], fbuf.at[p], sems.at[p, 1]),
                )
            )
        for pair in copies:
            for copy in pair:
                copy.start()
        k_iota = lax.broadcasted_iota(jnp.int32, (slots, LANES), 0)
        for p, pair in enumerate(copies):
            live = (k_iota < count_ref[jnp.bitwise_xor(e, p)]).astype(jnp.float32)
            for copy in pair:
                copy.wait()
            for j in range(rows):
                at = pl.ds(j * LANES, LANES)
                mask = fbuf[p, :, at].astype(jnp.float32) * live
                outs[p][0, pl.ds(j, slots, stride=rows), :] = mbuf[p, :, at] * mask
                outs[p][1, pl.ds(j, slots, stride=rows), :] = mask

    n = n_e * slots * lanes
    return pl.pallas_call(
        kernel,
        in_specs=[pl.BlockSpec(memory_space=pltpu.SMEM)] + [in_place()] * 2,
        out_specs=[whole()] * n_e,
        out_shape=[pltpu.VMEM((2, slots * rows, LANES), jnp.float32)] * n_e,
        scratch_shapes=[
            pltpu.VMEM((n_e, slots, lanes), morph.dtype),
            pltpu.VMEM((n_e, slots, lanes), footprint.dtype),
            pltpu.SemaphoreType.DMA((n_e, 2)),
        ],
        compiler_params=params(),
        cost_estimate=cost(n * 2, n * 16),
        name="pack",
    )(counts, morph, footprint)


def coadd_kernel(pieces, bands, n_e):
    n_b = len(pieces)
    rows = pieces[0].shape[1]
    total = n_b * rows
    per_e = total // n_e

    def kernel(*refs):
        ins, cov, outs, scr = refs[:n_b], refs[n_b], refs[n_b + 1 : n_b + 1 + n_e], refs[-1]
        e, b = lax.axis_index("epoch"), lax.axis_index("blend")
        parts = per_e // rows
        for m in range(n_b):
            at = jnp.bitwise_xor(b, m)
            block = jnp.bitwise_xor(at // parts, e)
            start = pl.multiple_of(block * per_e + (at % parts) * rows, 8)
            for band in range(bands):
                num, wsum = ins[m][band], ins[m][bands + band]
                inv = 1.0 / (1.0 + wsum)
                cov[band, pl.ds(start, rows), :] = wsum * inv
                scr[band, pl.ds(start, rows), :] = num * inv
        for p in range(n_e):
            for band in range(bands):
                outs[p][band] = scr[band, pl.ds(p * per_e, per_e), :]

    return pl.pallas_call(
        kernel,
        in_specs=[whole()] * n_b,
        out_specs=[whole()] * (1 + n_e),
        out_shape=[jax.ShapeDtypeStruct((bands, total, LANES), jnp.float32)]
        + [jax.ShapeDtypeStruct((bands, per_e, LANES), jnp.float32)] * n_e,
        scratch_shapes=[pltpu.VMEM((bands, total, LANES), jnp.float32)],
        compiler_params=params(),
        cost_estimate=cost(bands * total * LANES * 8, bands * total * LANES * 16),
        name="coadd",
    )(*pieces)


def deblend_kernel(counts, cov, coadds, packed, spectra):
    n_e = len(coadds)
    bands, total, _ = cov.shape
    per_e = total // n_e
    lanes = per_e * LANES
    slots = packed[0].shape[1] // per_e
    groups = total // 8

    def kernel(count_ref, cov_ref, *refs):
        co_in, pk_in = refs[:n_e], refs[n_e : 2 * n_e]
        spec_ref = refs[2 * n_e]
        outs = refs[2 * n_e + 1 : 3 * n_e + 1]
        co, mo, ma, res, acc, spec, step = refs[3 * n_e + 1 :]
        e = lax.axis_index("epoch")
        n_live = count_ref[e].astype(jnp.float32)
        k_iota = lax.broadcasted_iota(jnp.int32, (slots, LANES), 0)
        for p in range(n_e):
            for band in range(bands):
                co[band, pl.ds(p * per_e, per_e), :] = co_in[p][band]
            for k in range(slots):
                at = pl.ds(k * total + p * per_e, per_e)
                mo[at, :] = pk_in[p][0, pl.ds(k * per_e, per_e), :]
                ma[at, :] = pk_in[p][1, pl.ds(k * per_e, per_e), :]
        lane = lax.broadcasted_iota(jnp.int32, (slots, LANES), 1)
        small = (slots, spec_ref.shape[2])
        diag = lax.broadcasted_iota(jnp.int32, small, 0) == lax.broadcasted_iota(jnp.int32, small, 1)
        for c in range(bands):
            row = jnp.broadcast_to(spec_ref[c, pl.ds(e, 1), :], small)
            col = jnp.sum(jnp.where(diag, row, 0.0), axis=1, keepdims=True)
            spec[pl.ds(c * slots, slots), :] = jnp.broadcast_to(col, (slots, LANES))

        def bcast(ref, row):
            return jnp.broadcast_to(ref[pl.ds(row, 1), :], (8, LANES))

        for _ in range(ITERS):
            square = None
            for band in range(bands):
                s = spec[pl.ds(band * slots, slots), :]
                square = s * s if square is None else square + s * s
            step[...] = 1.0 / (1.0 + n_live * square)

            def group(g, carry):
                at = pl.multiple_of(g * 8, 8)
                m = [mo[pl.ds(pl.multiple_of(k * total + at, 8), 8), :] for k in range(slots)]
                cv = [cov_ref[c, pl.ds(at, 8), :] for c in range(bands)]
                cd = [co[c, pl.ds(at, 8), :] for c in range(bands)]
                r = []
                for c in range(bands):
                    model = None
                    for k in range(slots):
                        t = bcast(spec, c * slots + k) * m[k]
                        model = t if model is None else model + t
                    r.append(cv[c] * (cd[c] - model))
                for k in range(slots):
                    grad = None
                    for c in range(bands):
                        t = bcast(spec, c * slots + k) * r[c]
                        grad = t if grad is None else grad + t
                    mk = ma[pl.ds(pl.multiple_of(k * total + at, 8), 8), :]
                    m[k] = jnp.maximum(0.0, m[k] + grad * bcast(step, k)) * mk
                    mo[pl.ds(pl.multiple_of(k * total + at, 8), 8), :] = m[k]
                for c in range(bands):
                    model = None
                    for k in range(slots):
                        t = bcast(spec, c * slots + k) * m[k]
                        model = t if model is None else model + t
                    res[c, pl.ds(at, 8), :] = cv[c] * (cd[c] - model)
                return carry

            lax.fori_loop(0, groups, group, 0, unroll=2)
            for k in range(slots):
                sums = [None] * (bands + 1)
                for g in range(groups):
                    m = mo[pl.ds(k * total + g * 8, 8), :]
                    for c in range(bands):
                        t = m * res[c, pl.ds(g * 8, 8), :]
                        sums[c] = t if sums[c] is None else sums[c] + t
                    t = m * m
                    sums[bands] = t if sums[bands] is None else sums[bands] + t
                for c in range(bands + 1):
                    acc[pl.ds((c * slots + k) * 8, 8), :] = sums[c]

            def reduced(c):
                v = None
                for s in range(8):
                    t = acc[pl.ds(c * slots * 8 + s, slots, stride=8), :]
                    v = t if v is None else v + t
                return jnp.broadcast_to(jnp.sum(v, axis=1, keepdims=True), (slots, LANES))

            den = 1.0 + n_live * reduced(bands)
            for c in range(bands):
                s = spec[pl.ds(c * slots, slots), :]
                spec[pl.ds(c * slots, slots), :] = jnp.maximum(0.0, s + reduced(c) / den)

        tile = jnp.zeros((slots, LANES), jnp.float32)
        for c in range(bands):
            on_diag = jnp.where(lane == k_iota, spec[pl.ds(c * slots, slots), :], 0.0)
            row = jnp.broadcast_to(jnp.sum(on_diag, axis=0, keepdims=True), (slots, LANES))
            tile = jnp.where(k_iota == c, row, tile)
        for p in range(n_e):
            for j in range(per_e):
                at = pl.ds(p * per_e + j, slots, stride=total)
                outs[p][:, pl.ds(j * LANES, LANES)] = mo[at, :]
            outs[p][:, pl.ds(lanes, LANES)] = tile

    f32 = jnp.float32
    return pl.pallas_call(
        kernel,
        in_specs=[pl.BlockSpec(memory_space=pltpu.SMEM)] + [whole()] * (2 * n_e + 2),
        out_specs=[whole()] * n_e,
        out_shape=[jax.ShapeDtypeStruct((slots, lanes + LANES), f32)] * n_e,
        scratch_shapes=[
            pltpu.VMEM((bands, total, LANES), f32),
            pltpu.VMEM((slots * total, LANES), f32),
            pltpu.VMEM((slots * total, LANES), f32),
            pltpu.VMEM((bands, total, LANES), f32),
            pltpu.VMEM(((bands + 1) * slots * 8, LANES), f32),
            pltpu.VMEM((bands * slots, LANES), f32),
            pltpu.VMEM((slots, LANES), f32),
        ],
        compiler_params=params(),
        cost_estimate=cost(total * LANES * slots * bands * 8 * ITERS, total * LANES * 4 * 30),
        name="deblend",
    )(counts, cov, *coadds, *packed, spectra)


def place_coadd(pieces):
    n_e = len(pieces)
    bands, rows, _ = pieces[0].shape

    def kernel(*refs):
        ins, out, scr = refs[:n_e], refs[n_e], refs[n_e + 1]
        e = lax.axis_index("epoch")
        for p in range(n_e):
            scr[jnp.bitwise_xor(e, p)] = ins[p][...].reshape(bands * rows, LANES)
        for band in range(bands):
            for j in range(rows):
                for q in range(n_e):
                    out[band, q : q + 1, pl.ds(j * LANES, LANES)] = scr[q, pl.ds(band * rows + j, 1), :]

    return pl.pallas_call(
        kernel,
        in_specs=[whole()] * n_e,
        out_specs=whole(),
        out_shape=jax.ShapeDtypeStruct((bands, n_e, rows * LANES), jnp.float32),
        scratch_shapes=[pltpu.VMEM((n_e, bands * rows, LANES), jnp.float32)],
        compiler_params=params(),
        cost_estimate=cost(bands * n_e * rows * LANES, bands * n_e * rows * LANES * 8),
        name="place_coadd",
    )(*pieces)


def place_morph(pieces, bands):
    n_e = len(pieces)
    slots, lanes = pieces[0].shape
    lanes -= LANES

    def kernel(*refs):
        ins, out, spec, scr = refs[:n_e], refs[n_e], refs[n_e + 1], refs[n_e + 2]
        e = lax.axis_index("epoch")
        for p in range(n_e):
            q = jnp.bitwise_xor(e, p)
            out[q] = ins[p][:, 0:lanes]
            scr[q] = ins[p][:, lanes : lanes + LANES]
        for c in range(bands):
            for q in range(n_e):
                spec[c, q : q + 1, :] = scr[q, pl.ds(c, 1), 0:slots]

    return pl.pallas_call(
        kernel,
        in_specs=[whole()] * n_e,
        out_specs=[whole()] * 2,
        out_shape=[
            jax.ShapeDtypeStruct((n_e, slots, lanes), jnp.float32),
            jax.ShapeDtypeStruct((bands, n_e, slots), jnp.float32),
        ],
        scratch_shapes=[pltpu.VMEM((n_e, slots, LANES), jnp.float32)],
        compiler_params=params(),
        cost_estimate=cost(n_e * slots * lanes, n_e * slots * lanes * 8),
        name="place_morph",
    )(*pieces)


def xor_permute(x, axis, size, mask):
    return lax.ppermute(x, axis, [(i, i ^ mask) for i in range(size)])


def on_device_blend(
    n_e, n_b, visit_flux, visit_precision, visit_live, footprint, source_count, spectra_init, morphology_init
):
    owned, _, _ = morphology_init.shape
    bands = visit_flux.shape[2]
    cores = 2
    flux = jnp.transpose(visit_flux, (0, 2, 1, 3))
    prec = jnp.transpose(visit_precision, (0, 2, 1, 3))


    def swap(xs):
        out = [xs[0]]
        for p in range(1, n_e):
            out.append(xor_permute(xs[p], "epoch", n_e, p))
        return out

    spectra = jnp.transpose(spectra_init, (2, 0, 1))

    chips = n_b // cores
    chunks = [[k] for k in range(chips - 1, 1, -1)] + [[1, 0] if chips > 1 else [0]]
    pieces = [None] * n_b
    for n, ks in enumerate(chunks):
        s0, k0, s1, k1 = visit_sums(flux, prec, visit_live, ks, owned, n_e, cores, n > 0)
        for d, (send, keep, first, second) in enumerate(((s0, k0, 1, 2), (s1, k1, 2, 1))):
            got = xor_permute(send, "epoch", n_e, first)
            part, onward = halve_kernel(keep, got)
            got = xor_permute(onward, "epoch", n_e, second)
            full = finish_kernel(part, got)
            for i, k in enumerate(ks):
                m = k * cores + d
                pieces[m] = xor_permute(full[i], "blend", n_b, m) if m else full[i]
    packed = pack_kernel(source_count, hbm(morphology_init), hbm(footprint), n_e)
    packed = swap(packed)
    cov, *coadds = coadd_kernel(pieces, bands, n_e)
    blocks = deblend_kernel(source_count, cov, coadds, packed, spectra)
    out_coadd = place_coadd(swap(coadds))
    out_morph, out_spec = place_morph(swap(blocks), bands)
    return (jnp.transpose(out_coadd, (1, 0, 2)), jnp.transpose(out_spec, (1, 2, 0)), out_morph)


def solution(mesh):
    n_e, n_b = mesh.shape["epoch"], mesh.shape["blend"]
    in_specs = (
        P("epoch", None, None, "blend"),
        P("epoch", None, None, "blend"),
        P("epoch", None),
        P("blend", None, "epoch"),
        P("blend"),
        P("blend", None, None),
        P("blend", None, "epoch"),
    )
    out_specs = (P("blend", None, "epoch"), P("blend", None, None), P("blend", None, "epoch"))

    def on_device(*args):
        owned, slots, pix_part = args[6].shape
        pix = args[0].shape[3]
        by_blend = (
            n_e == 4
            and owned == n_e
            and slots == 8
            and n_b % 2 == 0
            and n_b & (n_b - 1) == 0
            and pix % (8 * LANES) == 0
            and pix_part % pix == 0
            and pix_part % (8 * LANES) == 0
        )
        if by_blend:
            return on_device_blend(n_e, n_b, *args)
        return on_device_general(*args)

    return jax.shard_map(
        on_device, mesh=mesh, in_specs=in_specs, out_specs=out_specs, check_vma=False
    )
```

```python
import jax
import jax.numpy as jnp
from jax import lax
from jax.experimental import pallas as pl
from jax.experimental.pallas import tpu as pltpu
from jax.sharding import PartitionSpec as P


ITERS = 2
LANES = 128


def on_device_general(
    visit_flux, visit_precision, visit_live, footprint, source_count, spectra_init, morphology_init
):
    weights = visit_precision.astype(jnp.float32) * visit_live.astype(jnp.float32)[:, :, None, None]
    numerator = jnp.sum(weights * visit_flux.astype(jnp.float32), axis=0)
    weight_sum = jnp.sum(weights, axis=0)
    pix_part = morphology_init.shape[2]
    owned = morphology_init.shape[0]
    numerator, weight_sum = (
        lax.psum_scatter(numerator, "epoch", scatter_dimension=2, tiled=True),
        lax.psum_scatter(weight_sum, "epoch", scatter_dimension=2, tiled=True),
    )
    every_blend, band_count, piece = numerator.shape
    numerator = numerator.reshape(every_blend, band_count, 1, piece)
    weight_sum = weight_sum.reshape(every_blend, band_count, 1, piece)
    numerator, weight_sum = (
        lax.all_to_all(numerator, "blend", split_axis=0, concat_axis=2, tiled=True),
        lax.all_to_all(weight_sum, "blend", split_axis=0, concat_axis=2, tiled=True),
    )
    blocks = numerator.shape[2]
    numerator = numerator.reshape(owned, band_count, blocks, 1, piece)
    weight_sum = weight_sum.reshape(owned, band_count, blocks, 1, piece)
    numerator, weight_sum = (
        lax.all_to_all(numerator, "epoch", split_axis=2, concat_axis=3, tiled=True),
        lax.all_to_all(weight_sum, "epoch", split_axis=2, concat_axis=3, tiled=True),
    )
    numerator = numerator.reshape(owned, band_count, pix_part)
    weight_sum = weight_sum.reshape(owned, band_count, pix_part)
    coadd_flux = numerator / (1.0 + weight_sum)
    coverage = weight_sum / (1.0 + weight_sum)
    slots = footprint.shape[1]
    source_live = (jnp.arange(slots, dtype=jnp.int32)[None, :] < source_count[:, None]).astype(
        jnp.float32
    )
    footprint_mask = footprint.astype(jnp.float32) * source_live[:, :, None]
    live_count = source_count.astype(jnp.float32)
    morphology = morphology_init * footprint_mask
    spectra = spectra_init
    highest = lax.Precision.HIGHEST
    for _ in range(ITERS):
        blend_model = jnp.einsum("bkc,bkp->bcp", spectra, morphology, precision=highest)
        residual = coverage * (coadd_flux - blend_model)
        morph_grad = jnp.einsum("bkc,bcp->bkp", spectra, residual, precision=highest)
        morph_step = 1.0 / (1.0 + live_count[:, None] * jnp.sum(spectra * spectra, axis=2))
        morphology = (
            jnp.maximum(0.0, morphology + morph_grad * morph_step[:, :, None]) * footprint_mask
        )
        blend_model = jnp.einsum("bkc,bkp->bcp", spectra, morphology, precision=highest)
        residual = coverage * (coadd_flux - blend_model)
        spectra_grad = jnp.einsum("bkp,bcp->bkc", morphology, residual, precision=highest)
        morph_norm = jnp.sum(morphology * morphology, axis=2)
        spectra_grad, morph_norm = lax.psum((spectra_grad, morph_norm), "epoch")
        spectra = jnp.maximum(
            0.0, spectra + spectra_grad / (1.0 + live_count[:, None] * morph_norm)[:, :, None]
        )
    return (coadd_flux, spectra, morphology)


VMEM_LIMIT = 6 * 1024 * 1024
SMALL_LIMIT = 1024 * 1024


def hbm(x):
    return pltpu.with_memory_space_constraint(x, pltpu.HBM)


def vmem(x):
    return pltpu.with_memory_space_constraint(x, pltpu.VMEM)


def whole():
    return pl.BlockSpec(memory_space=pltpu.VMEM)


def in_place():
    return pl.BlockSpec(memory_space=pltpu.HBM)


def cost(flops, nbytes):
    return pl.CostEstimate(flops=int(flops), bytes_accessed=int(nbytes), transcendentals=0)


def params(limit=VMEM_LIMIT):
    return pltpu.CompilerParams(vmem_limit_bytes=limit)


def visit_sums(flux, prec, live, ks, owned, n_e, cores, fetched):
    epochs, bands, blends, pix = flux.shape
    group = cores * owned
    rows = pix // LANES
    block_rows = 2 * bands * rows
    half = n_e // 2
    n_k = len(ks)
    order = {0: ((1, 3), (0, 2)), 1: ((2, 3), (0, 1))}

    def kernel(live_in, flux_in, prec_in, s0, k0, s1, k1, scr, *own):
        e, b = lax.axis_index("epoch"), lax.axis_index("blend")
        chip, c = b // cores, b % cores

        def at_rows(i):
            return pl.ds(pl.multiple_of((chip ^ ks[i]) * group, 8), group)

        if fetched:
            live_ref = live_in

            def load(ref, i, band, ep, at):
                return ref[ep, band, at_rows(i), at].astype(jnp.float32)

            refs = (flux_in, prec_in)
        else:
            fbuf, pbuf, live_ref, sems, live_sem = own

            def copies(i, band):
                return [
                    pltpu.make_async_copy(ref.at[:, band, at_rows(i), :], buf.at[i, band], sems.at[i, band, n])
                    for n, (ref, buf) in enumerate(((flux_in, fbuf), (prec_in, pbuf)))
                ]

            live_copy = pltpu.make_async_copy(live_in, live_ref, live_sem)
            live_copy.start(priority=1)
            for i in range(n_k):
                for band in range(bands):
                    for n, copy in enumerate(copies(i, band)):
                        copy.start(priority=n)
            live_copy.wait()

            def load(ref, i, band, ep, at):
                return ref[i, band, ep, :, at].astype(jnp.float32)

            refs = (fbuf, pbuf)
        sub = lax.broadcasted_iota(jnp.int32, (group, blends), 0)
        lane = lax.broadcasted_iota(jnp.int32, (group, blends), 1)
        for i in range(n_k):
            pick = lane == sub + (chip ^ ks[i]) * group
            lives = []
            for ep in range(epochs):
                row = live_ref[ep : ep + 1, :].astype(jnp.float32)
                col = jnp.where(pick, jnp.broadcast_to(row, pick.shape), 0.0)
                lives.append(jnp.broadcast_to(jnp.sum(col, axis=1, keepdims=True), (group, LANES)))
            for band in range(bands):
                if not fetched:
                    for copy in copies(i, band):
                        copy.wait()
                for j in range(rows):
                    at = pl.ds(j * LANES, LANES)
                    num = wsum = None
                    for ep in range(epochs):
                        w = load(refs[1], i, band, ep, at) * lives[ep]
                        n = w * load(refs[0], i, band, ep, at)
                        num = n if num is None else num + n
                        wsum = w if wsum is None else wsum + w
                    scr[pl.ds(band * rows + j, group, stride=block_rows), :] = num
                    scr[pl.ds((bands + band) * rows + j, group, stride=block_rows), :] = wsum
            for d, outs in ((0, (s0, k0)), (1, (s1, k1))):
                for ref, slots in zip(outs, order[d]):
                    for slot, p in enumerate(slots):
                        r = jnp.bitwise_xor(c, d) * n_e + jnp.bitwise_xor(e, p)
                        start = pl.multiple_of(r * block_rows, 8)
                        ref[slot, i] = scr[pl.ds(start, block_rows), :].reshape(2 * bands, rows, LANES)

    scratch = [pltpu.VMEM((group * block_rows, LANES), jnp.float32)]
    if not fetched:
        scratch += [
            pltpu.VMEM((n_k, bands, epochs, group, pix), flux.dtype),
            pltpu.VMEM((n_k, bands, epochs, group, pix), prec.dtype),
            pltpu.VMEM(live.shape, live.dtype),
            pltpu.SemaphoreType.DMA((n_k, bands, 2)),
            pltpu.SemaphoreType.DMA,
        ]
    out = pltpu.VMEM((half, n_k, 2 * bands, rows, LANES), jnp.float32)
    n_in = n_k * epochs * bands * group * pix
    put = vmem if fetched else hbm
    return pl.pallas_call(
        kernel,
        in_specs=[whole() if fetched else in_place()] * 3,
        out_specs=[whole()] * 4,
        out_shape=[out] * 4,
        scratch_shapes=scratch,
        compiler_params=params(),
        cost_estimate=cost(n_in * 6, n_in * 4 + n_in * 2),
        name="visit_sums",
    )(put(live), put(flux), put(prec))


def halve_kernel(keep, got):
    def kernel(keep_ref, got_ref, part, onward):
        part[...] = keep_ref[0] + got_ref[0]
        onward[...] = keep_ref[1] + got_ref[1]

    out = pltpu.VMEM(keep.shape[1:], keep.dtype)
    return pl.pallas_call(
        kernel,
        in_specs=[whole()] * 2,
        out_specs=[whole()] * 2,
        out_shape=[out] * 2,
        compiler_params=params(SMALL_LIMIT),
        cost_estimate=cost(keep.size, keep.size * 12),
        name="halve",
    )(keep, vmem(got))


def finish_kernel(part, got):
    n_k = part.shape[0]

    def kernel(part_ref, got_ref, *outs):
        for i in range(n_k):
            outs[i][...] = part_ref[i] + got_ref[i]

    return pl.pallas_call(
        kernel,
        in_specs=[whole()] * 2,
        out_specs=[whole()] * n_k,
        out_shape=[pltpu.VMEM(part.shape[1:], part.dtype)] * n_k,
        compiler_params=params(SMALL_LIMIT),
        cost_estimate=cost(part.size, part.size * 12),
        name="finish",
    )(part, vmem(got))


def pack_kernel(counts, morph, footprint, n_e):
    _, slots, lanes = morph.shape
    rows = lanes // LANES

    def kernel(count_ref, morph_ref, foot_ref, *refs):
        outs, mbuf, fbuf, sems = refs[:n_e], refs[n_e], refs[n_e + 1], refs[n_e + 2]
        e = lax.axis_index("epoch")
        copies = []
        for p in range(n_e):
            q = jnp.bitwise_xor(e, p)
            copies.append(
                (
                    pltpu.make_async_copy(morph_ref.at[q], mbuf.at[p], sems.at[p, 0]),
                    pltpu.make_async_copy(foot_ref.at[q], fbuf.at[p], sems.at[p, 1]),
                )
            )
        for pair in copies:
            for copy in pair:
                copy.start()
        k_iota = lax.broadcasted_iota(jnp.int32, (slots, LANES), 0)
        for p, pair in enumerate(copies):
            live = (k_iota < count_ref[jnp.bitwise_xor(e, p)]).astype(jnp.float32)
            for copy in pair:
                copy.wait()
            for j in range(rows):
                at = pl.ds(j * LANES, LANES)
                mask = fbuf[p, :, at].astype(jnp.float32) * live
                outs[p][0, pl.ds(j, slots, stride=rows), :] = mbuf[p, :, at] * mask
                outs[p][1, pl.ds(j, slots, stride=rows), :] = mask

    n = n_e * slots * lanes
    return pl.pallas_call(
        kernel,
        in_specs=[pl.BlockSpec(memory_space=pltpu.SMEM)] + [in_place()] * 2,
        out_specs=[whole()] * n_e,
        out_shape=[pltpu.VMEM((2, slots * rows, LANES), jnp.float32)] * n_e,
        scratch_shapes=[
            pltpu.VMEM((n_e, slots, lanes), morph.dtype),
            pltpu.VMEM((n_e, slots, lanes), footprint.dtype),
            pltpu.SemaphoreType.DMA((n_e, 2)),
        ],
        compiler_params=params(),
        cost_estimate=cost(n * 2, n * 16),
        name="pack",
    )(counts, morph, footprint)


def coadd_kernel(pieces, bands, n_e):
    n_b = len(pieces)
    rows = pieces[0].shape[1]
    total = n_b * rows
    per_e = total // n_e

    def kernel(*refs):
        ins, cov, outs, scr = refs[:n_b], refs[n_b], refs[n_b + 1 : n_b + 1 + n_e], refs[-1]
        e, b = lax.axis_index("epoch"), lax.axis_index("blend")
        parts = per_e // rows
        for m in range(n_b):
            at = jnp.bitwise_xor(b, m)
            block = jnp.bitwise_xor(at // parts, e)
            start = pl.multiple_of(block * per_e + (at % parts) * rows, 8)
            for band in range(bands):
                num, wsum = ins[m][band], ins[m][bands + band]
                inv = 1.0 / (1.0 + wsum)
                cov[band, pl.ds(start, rows), :] = wsum * inv
                scr[band, pl.ds(start, rows), :] = num * inv
        for p in range(n_e):
            for band in range(bands):
                outs[p][band] = scr[band, pl.ds(p * per_e, per_e), :]

    return pl.pallas_call(
        kernel,
        in_specs=[whole()] * n_b,
        out_specs=[whole()] * (1 + n_e),
        out_shape=[jax.ShapeDtypeStruct((bands, total, LANES), jnp.float32)]
        + [jax.ShapeDtypeStruct((bands, per_e, LANES), jnp.float32)] * n_e,
        scratch_shapes=[pltpu.VMEM((bands, total, LANES), jnp.float32)],
        compiler_params=params(),
        cost_estimate=cost(bands * total * LANES * 8, bands * total * LANES * 16),
        name="coadd",
    )(*pieces)


def deblend_kernel(counts, cov, coadds, packed, spectra):
    n_e = len(coadds)
    bands, total, _ = cov.shape
    per_e = total // n_e
    lanes = per_e * LANES
    slots = packed[0].shape[1] // per_e
    groups = total // 8

    def kernel(count_ref, cov_ref, *refs):
        co_in, pk_in = refs[:n_e], refs[n_e : 2 * n_e]
        spec_ref = refs[2 * n_e]
        outs = refs[2 * n_e + 1 : 3 * n_e + 1]
        co, mo, ma, res, acc, spec, step = refs[3 * n_e + 1 :]
        e = lax.axis_index("epoch")
        n_live = count_ref[e].astype(jnp.float32)
        k_iota = lax.broadcasted_iota(jnp.int32, (slots, LANES), 0)
        for p in range(n_e):
            for band in range(bands):
                co[band, pl.ds(p * per_e, per_e), :] = co_in[p][band]
            for k in range(slots):
                at = pl.ds(k * total + p * per_e, per_e)
                mo[at, :] = pk_in[p][0, pl.ds(k * per_e, per_e), :]
                ma[at, :] = pk_in[p][1, pl.ds(k * per_e, per_e), :]
        lane = lax.broadcasted_iota(jnp.int32, (slots, LANES), 1)
        small = (slots, spec_ref.shape[2])
        diag = lax.broadcasted_iota(jnp.int32, small, 0) == lax.broadcasted_iota(jnp.int32, small, 1)
        for c in range(bands):
            row = jnp.broadcast_to(spec_ref[c, pl.ds(e, 1), :], small)
            col = jnp.sum(jnp.where(diag, row, 0.0), axis=1, keepdims=True)
            spec[pl.ds(c * slots, slots), :] = jnp.broadcast_to(col, (slots, LANES))

        def bcast(ref, row):
            return jnp.broadcast_to(ref[pl.ds(row, 1), :], (8, LANES))

        for _ in range(ITERS):
            square = None
            for band in range(bands):
                s = spec[pl.ds(band * slots, slots), :]
                square = s * s if square is None else square + s * s
            step[...] = 1.0 / (1.0 + n_live * square)

            def group(g, carry):
                at = pl.multiple_of(g * 8, 8)
                m = [mo[pl.ds(pl.multiple_of(k * total + at, 8), 8), :] for k in range(slots)]
                cv = [cov_ref[c, pl.ds(at, 8), :] for c in range(bands)]
                cd = [co[c, pl.ds(at, 8), :] for c in range(bands)]
                r = []
                for c in range(bands):
                    model = None
                    for k in range(slots):
                        t = bcast(spec, c * slots + k) * m[k]
                        model = t if model is None else model + t
                    r.append(cv[c] * (cd[c] - model))
                for k in range(slots):
                    grad = None
                    for c in range(bands):
                        t = bcast(spec, c * slots + k) * r[c]
                        grad = t if grad is None else grad + t
                    mk = ma[pl.ds(pl.multiple_of(k * total + at, 8), 8), :]
                    m[k] = jnp.maximum(0.0, m[k] + grad * bcast(step, k)) * mk
                    mo[pl.ds(pl.multiple_of(k * total + at, 8), 8), :] = m[k]
                for c in range(bands):
                    model = None
                    for k in range(slots):
                        t = bcast(spec, c * slots + k) * m[k]
                        model = t if model is None else model + t
                    res[c, pl.ds(at, 8), :] = cv[c] * (cd[c] - model)
                return carry

            lax.fori_loop(0, groups, group, 0, unroll=2)
            for k in range(slots):
                sums = [None] * (bands + 1)
                for g in range(groups):
                    m = mo[pl.ds(k * total + g * 8, 8), :]
                    for c in range(bands):
                        t = m * res[c, pl.ds(g * 8, 8), :]
                        sums[c] = t if sums[c] is None else sums[c] + t
                    t = m * m
                    sums[bands] = t if sums[bands] is None else sums[bands] + t
                for c in range(bands + 1):
                    acc[pl.ds((c * slots + k) * 8, 8), :] = sums[c]

            def reduced(c):
                v = None
                for s in range(8):
                    t = acc[pl.ds(c * slots * 8 + s, slots, stride=8), :]
                    v = t if v is None else v + t
                return jnp.broadcast_to(jnp.sum(v, axis=1, keepdims=True), (slots, LANES))

            den = 1.0 + n_live * reduced(bands)
            for c in range(bands):
                s = spec[pl.ds(c * slots, slots), :]
                spec[pl.ds(c * slots, slots), :] = jnp.maximum(0.0, s + reduced(c) / den)

        tile = jnp.zeros((slots, LANES), jnp.float32)
        for c in range(bands):
            on_diag = jnp.where(lane == k_iota, spec[pl.ds(c * slots, slots), :], 0.0)
            row = jnp.broadcast_to(jnp.sum(on_diag, axis=0, keepdims=True), (slots, LANES))
            tile = jnp.where(k_iota == c, row, tile)
        for p in range(n_e):
            for j in range(per_e):
                at = pl.ds(p * per_e + j, slots, stride=total)
                outs[p][:, pl.ds(j * LANES, LANES)] = mo[at, :]
            outs[p][:, pl.ds(lanes, LANES)] = tile

    f32 = jnp.float32
    return pl.pallas_call(
        kernel,
        in_specs=[pl.BlockSpec(memory_space=pltpu.SMEM)] + [whole()] * (2 * n_e + 2),
        out_specs=[whole()] * n_e,
        out_shape=[jax.ShapeDtypeStruct((slots, lanes + LANES), f32)] * n_e,
        scratch_shapes=[
            pltpu.VMEM((bands, total, LANES), f32),
            pltpu.VMEM((slots * total, LANES), f32),
            pltpu.VMEM((slots * total, LANES), f32),
            pltpu.VMEM((bands, total, LANES), f32),
            pltpu.VMEM(((bands + 1) * slots * 8, LANES), f32),
            pltpu.VMEM((bands * slots, LANES), f32),
            pltpu.VMEM((slots, LANES), f32),
        ],
        compiler_params=params(),
        cost_estimate=cost(total * LANES * slots * bands * 8 * ITERS, total * LANES * 4 * 30),
        name="deblend",
    )(counts, cov, *coadds, *packed, spectra)


def place_coadd(pieces):
    n_e = len(pieces)
    bands, rows, _ = pieces[0].shape

    def kernel(*refs):
        ins, out, scr = refs[:n_e], refs[n_e], refs[n_e + 1]
        e = lax.axis_index("epoch")
        for p in range(n_e):
            scr[jnp.bitwise_xor(e, p)] = ins[p][...].reshape(bands * rows, LANES)
        for band in range(bands):
            for j in range(rows):
                for q in range(n_e):
                    out[band, q : q + 1, pl.ds(j * LANES, LANES)] = scr[q, pl.ds(band * rows + j, 1), :]

    return pl.pallas_call(
        kernel,
        in_specs=[whole()] * n_e,
        out_specs=whole(),
        out_shape=jax.ShapeDtypeStruct((bands, n_e, rows * LANES), jnp.float32),
        scratch_shapes=[pltpu.VMEM((n_e, bands * rows, LANES), jnp.float32)],
        compiler_params=params(),
        cost_estimate=cost(bands * n_e * rows * LANES, bands * n_e * rows * LANES * 8),
        name="place_coadd",
    )(*pieces)


def place_morph(pieces, bands):
    n_e = len(pieces)
    slots, lanes = pieces[0].shape
    lanes -= LANES

    def kernel(*refs):
        ins, out, spec, scr = refs[:n_e], refs[n_e], refs[n_e + 1], refs[n_e + 2]
        e = lax.axis_index("epoch")
        for p in range(n_e):
            q = jnp.bitwise_xor(e, p)
            out[q] = ins[p][:, 0:lanes]
            scr[q] = ins[p][:, lanes : lanes + LANES]
        for c in range(bands):
            for q in range(n_e):
                spec[c, q : q + 1, :] = scr[q, pl.ds(c, 1), 0:slots]

    return pl.pallas_call(
        kernel,
        in_specs=[whole()] * n_e,
        out_specs=[whole()] * 2,
        out_shape=[
            jax.ShapeDtypeStruct((n_e, slots, lanes), jnp.float32),
            jax.ShapeDtypeStruct((bands, n_e, slots), jnp.float32),
        ],
        scratch_shapes=[pltpu.VMEM((n_e, slots, LANES), jnp.float32)],
        compiler_params=params(),
        cost_estimate=cost(n_e * slots * lanes, n_e * slots * lanes * 8),
        name="place_morph",
    )(*pieces)


def xor_permute(x, axis, size, mask):
    return lax.ppermute(x, axis, [(i, i ^ mask) for i in range(size)])


def on_device_blend(
    n_e, n_b, visit_flux, visit_precision, visit_live, footprint, source_count, spectra_init, morphology_init
):
    owned, _, _ = morphology_init.shape
    bands = visit_flux.shape[2]
    cores = 2
    flux = jnp.transpose(visit_flux, (0, 2, 1, 3))
    prec = jnp.transpose(visit_precision, (0, 2, 1, 3))


    def swap(xs):
        out = [xs[0]]
        for p in range(1, n_e):
            out.append(xor_permute(xs[p], "epoch", n_e, p))
        return out

    spectra = jnp.transpose(spectra_init, (2, 0, 1))

    chips = n_b // cores
    chunks = [[k] for k in range(chips - 1, 1, -1)] + [[1, 0] if chips > 1 else [0]]
    pieces = [None] * n_b
    for n, ks in enumerate(chunks):
        s0, k0, s1, k1 = visit_sums(flux, prec, visit_live, ks, owned, n_e, cores, n > 0)
        for d, (send, keep, first, second) in enumerate(((s0, k0, 1, 2), (s1, k1, 2, 1))):
            got = xor_permute(send, "epoch", n_e, first)
            part, onward = halve_kernel(keep, got)
            got = xor_permute(onward, "epoch", n_e, second)
            full = finish_kernel(part, got)
            for i, k in enumerate(ks):
                m = k * cores + d
                pieces[m] = xor_permute(full[i], "blend", n_b, m) if m else full[i]
    packed = pack_kernel(source_count, hbm(morphology_init), hbm(footprint), n_e)
    packed = swap(packed)
    cov, *coadds = coadd_kernel(pieces, bands, n_e)
    blocks = deblend_kernel(source_count, cov, coadds, packed, spectra)
    out_coadd = place_coadd(swap(coadds))
    out_morph, out_spec = place_morph(swap(blocks), bands)
    return (jnp.transpose(out_coadd, (1, 0, 2)), jnp.transpose(out_spec, (1, 2, 0)), out_morph)


def solution(mesh):
    n_e, n_b = mesh.shape["epoch"], mesh.shape["blend"]
    in_specs = (
        P("epoch", None, None, "blend"),
        P("epoch", None, None, "blend"),
        P("epoch", None),
        P("blend", None, "epoch"),
        P("blend"),
        P("blend", None, None),
        P("blend", None, "epoch"),
    )
    out_specs = (P("blend", None, "epoch"), P("blend", None, None), P("blend", None, "epoch"))

    def on_device(*args):
        owned, slots, pix_part = args[6].shape
        pix = args[0].shape[3]
        by_blend = (
            n_e == 4
            and owned == n_e
            and slots == 8
            and n_b % 2 == 0
            and n_b & (n_b - 1) == 0
            and pix % (8 * LANES) == 0
            and pix_part % pix == 0
            and pix_part % (8 * LANES) == 0
        )
        if by_blend:
            return on_device_blend(n_e, n_b, *args)
        return on_device_general(*args)

    return jax.shard_map(
        on_device, mesh=mesh, in_specs=in_specs, out_specs=out_specs, check_vma=False
    )
```
